256 devices in a mesh: seq: 16 (over x, y_hi, core), head: 16 (over y_lo, z).
Axes of the slice: x: 4, y: 4 (y_hi: 2, y_lo: 2; y = y_hi * 2 + y_lo), z: 8, core: 2. Of those that a mesh axis runs over, the one named last changes fastest.
Arguments:
- tokens: bfloat16 [4096, 8192], P('seq', 'head'), may hold values from -12 to 12
- w_query: bfloat16 [8192, 4096], P(None, 'head'), may hold values from -0.100097656 to 0.100097656
- w_keyval: bfloat16 [8192, 512], P(None, 'head'), may hold values from -0.15039062 to 0.15039062
- w_out: bfloat16 [4096, 8192], P('head'), may hold values from -0.125 to 0.125
Outputs:
- layer_out: bfloat16 [4096, 8192], P('seq', 'head')
The draws below stay inside these ranges and needn't reach their ends.
All inputs are finite; a program needn't handle non-finite values.
Results may differ from the reference program's by a relative error of at most 0.0075.
The reference program's roundings to bfloat16 on the way (of `queries`, `keyval`, `product`, `weights` and `attended`) count: a program that leaves them out, or rounds other values in their place, can miss the bound.
Values may be sent and summed in bfloat16 or wider, within the bound.
No kernel may reach another device: no remote copies, remote signals or barrier semaphores. Data moves between devices by JAX's collectives and lax.ppermute only.
A program may use at most 64 MiB of HBM per device.

```python
import math
import jax
import jax.numpy as jnp
from jax import lax

D = 8192
HEADS = 32
HEAD = 128
WIN1 = 512
WIN2 = 32
TOK_DEV = 256
TOKENS = 4096
HD = 4096


def draw_tokens(key, part):
    noise = jax.random.normal(jax.random.fold_in(key, 1), (TOKENS, D), jnp.float32)
    return jnp.clip(noise, -6.0, 6.0).astype(jnp.bfloat16)


def draw_w_query(key, part):
    values = jax.random.normal(jax.random.fold_in(key, 11), (D, HEADS * HEAD), jnp.float32) / math.sqrt(D)
    values = jnp.clip(values, -6.0 / math.sqrt(D), 6.0 / math.sqrt(D))
    return jnp.clip(values, -0.1, 0.1).astype(jnp.bfloat16)


def draw_w_keyval(key, part):
    values = 1.7 * jax.random.normal(jax.random.fold_in(key, 21), (D, 4 * HEAD), jnp.float32) / math.sqrt(D)
    values = jnp.clip(values, -10.2 / math.sqrt(D), 10.2 / math.sqrt(D))
    return jnp.clip(values, -0.15, 0.15).astype(jnp.bfloat16)


def with_spikes(result, own_key, source, target, parts, factor):
    owner, partner = [(jnp.arange(result.shape[dim]) // (result.shape[dim] // parts)).reshape([-1 if axis == dim else 1 for axis in range(result.ndim)]) for dim in (source, target)]
    chosen = jax.random.permutation(own_key, parts)[partner]
    strong = (owner == chosen) | (owner == (partner + parts // 2) % parts)
    return jnp.where(strong, factor * result, result)


def levels(key, shape, shards, low, largest):
    factor_of = 1.0
    for dim, parts in shards:
        draws = jax.random.uniform(jax.random.fold_in(jax.random.fold_in(key, 6), dim), (parts,), jnp.float32, low / len(shards), largest / len(shards))
        factor_of = factor_of * jnp.repeat(jnp.exp(draws), shape[dim] // parts).reshape((-1,) + (1,) * (len(shape) - 1 - dim))
    return factor_of


def gaussian_with(own_key, shape, spread, bound, split, heavy, kind=jnp.bfloat16):
    array = spread * jax.random.normal(own_key, shape, jnp.float32)
    if split:
        array = array * levels(own_key, shape, split, -0.22, 0.18)
    return jnp.clip(with_spikes(array, jax.random.fold_in(own_key, 3), *heavy), -bound, bound).astype(kind)


def setup_inputs(seed: int = 0) -> dict:
    seeds = jax.random.split(jax.random.key(seed), 5)
    tokens = draw_tokens(jax.random.fold_in(seeds[4], 71), 0)
    w_query = draw_w_query(jax.random.fold_in(seeds[4], 71), 0)
    w_keyval = draw_w_keyval(jax.random.fold_in(seeds[4], 71), 0)
    w_out = gaussian_with(seeds[3], (HD, D), HD ** -0.5, 0.125, ((0, 16),), (0, 1, 16, 2.0))
    return {"tokens": tokens, "w_query": w_query, "w_keyval": w_keyval, "w_out": w_out}


def window_rows(source, window, amount):
    return jnp.stack([source[window - 1 - lag_index: window - 1 - lag_index + amount] for lag_index in range(window)], axis=1)


def attend_block(query_rows, key_rows, value_rows, second_keys, second_values, first_pos):
    amount = query_rows.shape[0]
    window = second_keys.shape[0] - amount + 1
    lead = key_rows.shape[0] - amount
    key_two = window_rows(second_keys, window, amount)
    value_two = window_rows(second_values, window, amount)
    product = (query_rows.astype(jnp.float32)[:, None, :] * key_two.astype(jnp.float32)).astype(jnp.bfloat16)
    scores = jnp.einsum("ird,jd->irj", product.astype(jnp.float32), key_rows.astype(jnp.float32), precision=lax.Precision.HIGHEST) * (HEAD ** -0.5)
    row_ids = jnp.arange(amount, dtype=jnp.int32)[:, None, None]
    lag_ids = jnp.arange(window, dtype=jnp.int32)[None, :, None]
    column = jnp.arange(amount + lead, dtype=jnp.int32)[None, None, :]
    usable = (column >= row_ids) & (column <= row_ids + lead) & (first_pos - lead + column >= 0) & (first_pos + row_ids - lag_ids >= 0)
    row_peak = jnp.max(jnp.where(usable, scores, -jnp.inf), axis=(1, 2))
    raised = jnp.where(usable, jnp.exp(scores - row_peak[:, None, None]), 0.0)
    row_total = jnp.sum(raised, axis=(1, 2))
    weights = raised.astype(jnp.bfloat16)
    mixture = jnp.einsum("irj,jd->ird", weights.astype(jnp.float32), value_rows.astype(jnp.float32), precision=lax.Precision.HIGHEST)
    combined = jnp.sum(mixture * value_two.astype(jnp.float32), axis=1)
    return (combined / row_total[:, None]).astype(jnp.bfloat16)


def reference(tokens, w_query, w_keyval, w_out):
    queries = jnp.dot(tokens, w_query, preferred_element_type=jnp.float32).astype(jnp.bfloat16)
    keyval = jnp.dot(tokens, w_keyval, preferred_element_type=jnp.float32).astype(jnp.bfloat16)
    lead = WIN1 - 1
    first_pad = jnp.concatenate([jnp.zeros((lead, 2 * HEAD), jnp.bfloat16), keyval[:, :2 * HEAD]], axis=0)
    second_pad = jnp.concatenate([jnp.zeros((WIN2 - 1, 2 * HEAD), jnp.bfloat16), keyval[:, 2 * HEAD:]], axis=0)
    block = min(TOK_DEV, 128)
    block_count = TOKENS // block

    def one_block(block_index):
        offset = (block_index * block).astype(jnp.int32)
        first_rows = lax.dynamic_slice_in_dim(first_pad, offset, block + lead, 0)
        second_rows = lax.dynamic_slice_in_dim(second_pad, offset, block + WIN2 - 1, 0)

        def one_head(head_index):
            column_start = (head_index * HEAD).astype(jnp.int32)
            query_rows = lax.dynamic_slice(queries, (offset, column_start), (block, HEAD))
            return attend_block(query_rows, first_rows[:, :HEAD], first_rows[:, HEAD:], second_rows[:, :HEAD], second_rows[:, HEAD:], offset)

        return lax.map(one_head, jnp.arange(HEADS, dtype=jnp.int32))

    stacked = lax.map(one_block, jnp.arange(block_count, dtype=jnp.int32))
    attended = jnp.transpose(stacked, (0, 2, 1, 3)).reshape(TOKENS, HEADS * HEAD)
    return jnp.dot(attended, w_out, preferred_element_type=jnp.float32).astype(jnp.bfloat16)
```

```python
import jax, jax.numpy as jnp, functools
from jax import lax
from jax.experimental import pallas as pl
from jax.experimental.pallas import tpu as pltpu
from jax.sharding import PartitionSpec as P
HEAD = 128
WIN1 = 512
WIN2 = 32
BLK = 128
def attend_kernel(group, seq_ref, q_ref, first_ref, second_ref, out_ref, k2f, v2f, kpair, vtile, s_scr, mx_scr, mcb_scr):
    heads = q_ref.shape[1] // HEAD
    blocks = q_ref.shape[0] // BLK
    seq = seq_ref[0]
    tok = q_ref.shape[0]
    coef = (HEAD ** -0.5) * 1.4426950408889634
    start = seq == 0
    k2f[...] = second_ref[:, :HEAD].astype(jnp.float32)
    v2f[...] = second_ref[:, HEAD:].astype(jnp.float32)

    @pl.when(start)
    def _():
        k2f[:WIN2] = jnp.broadcast_to(k2f[WIN2:WIN2 + 1], (WIN2, HEAD))
        v2f[:WIN2] = jnp.zeros((WIN2, HEAD), jnp.float32)

    row = lax.broadcasted_iota(jnp.int32, (BLK, BLK), 0)
    col = lax.broadcasted_iota(jnp.int32, (BLK, BLK), 1)
    early = col > row
    absent = jnp.maximum(WIN1 - seq * tok, 0) // BLK
    low = jnp.float32(-1e30)

    def one(combo, _):
        h = combo // blocks
        b = combo % blocks
        base = pl.multiple_of(b * BLK, BLK)
        hcol = pl.multiple_of(h * HEAD, HEAD)
        qf = q_ref[pl.ds(base, BLK), pl.ds(hcol, HEAD)].astype(jnp.float32)
        kpair[:BLK] = first_ref[pl.ds(base, BLK), :HEAD]
        kpair[BLK:2 * BLK] = first_ref[pl.ds(base + 4 * BLK, BLK), :HEAD]
        kpair[2 * BLK:] = first_ref[pl.ds(base + BLK, 3 * BLK), :HEAD]
        vtile[:BLK] = first_ref[pl.ds(base, BLK), HEAD:]
        vtile[BLK:2 * BLK] = first_ref[pl.ds(base + 4 * BLK, BLK), HEAD:]
        vtile[2 * BLK:] = first_ref[pl.ds(base + BLK, 3 * BLK), HEAD:]
        mx_scr[...] = jnp.full(mx_scr.shape, low, jnp.float32)

        def scores(step, _):
            lag0 = step * group
            prods = []
            for g in range(group):
                k2 = k2f[pl.ds(WIN2 + base - lag0 - g, BLK), :]
                prods.append((qf * k2).astype(jnp.bfloat16))
            prod = jnp.concatenate(prods, axis=0)
            dims = (((1,), (1,)), ((), ()))
            for t in range(3):
                width = 2 * BLK if t < 2 else BLK
                s = lax.dot_general(prod, kpair[2 * BLK * t: 2 * BLK * t + width], dims, preferred_element_type=jnp.float32)
                s = s.reshape(group, BLK, width)
                if t == 0:
                    parts = [(0, jnp.where(early[None], s[:, :, :BLK], s[:, :, BLK:]))]
                elif t == 1:
                    parts = [(1, s[:, :, :BLK]), (2, s[:, :, BLK:])]
                else:
                    parts = [(3, s)]
                for place, value in parts:
                    s_scr[pl.ds(lag0, group), :, place * BLK:(place + 1) * BLK] = value
                    top = value[0]
                    for g in range(1, group):
                        top = jnp.maximum(top, value[g])
                    mx_scr[place] = jnp.maximum(mx_scr[place], top)
            return 0

        lax.fori_loop(0, WIN2 // group, scores, 0)
        tops = []
        gone = []
        for place in range(4):
            hide = (b + place) < absent
            if place == 0:
                gone.append(jnp.logical_and(early, hide))
            else:
                gone.append(jnp.logical_and(row >= 0, hide))
            tops.append(jnp.where(gone[place], low, mx_scr[place]))
        peak = jnp.max(jnp.maximum(jnp.maximum(tops[0], tops[1]), jnp.maximum(tops[2], tops[3])), axis=1, keepdims=True) * coef
        for place in range(4):
            mcb_scr[place] = jnp.where(gone[place], -low, jnp.broadcast_to(peak, (BLK, BLK)))

        def mix(lag, carry):
            acc, tot = carry
            raised = [jnp.exp2(s_scr[lag, :, p * BLK:(p + 1) * BLK] * coef - mcb_scr[p]) for p in range(4)]
            tot = tot + ((raised[0] + raised[1]) + (raised[2] + raised[3]))
            w = jnp.concatenate([
                jnp.where(early, raised[0], 0.0).astype(jnp.bfloat16),
                jnp.where(early, 0.0, raised[0]).astype(jnp.bfloat16),
                raised[1].astype(jnp.bfloat16), raised[2].astype(jnp.bfloat16), raised[3].astype(jnp.bfloat16)], axis=1)
            m = jnp.dot(w, vtile[...], preferred_element_type=jnp.float32)
            acc = acc + m * v2f[pl.ds(WIN2 + base - lag, BLK), :]
            return acc, tot

        zero = jnp.zeros((BLK, HEAD), jnp.float32)
        acc, tot = lax.fori_loop(0, WIN2, mix, (zero, zero), unroll=4)
        last = [jnp.exp2(s_scr[WIN2 - 1, :, p * BLK:(p + 1) * BLK] * coef - mcb_scr[p]) for p in range(4)]
        twice = jnp.where(jnp.logical_and(start, b == 0), jnp.maximum(WIN2 - 1 - row, 0), 0).astype(jnp.float32)
        tot = tot - twice * ((last[0] + last[1]) + (last[2] + last[3]))
        total = jnp.sum(tot, axis=1, keepdims=True)
        out_ref[pl.ds(base, BLK), pl.ds(hcol, HEAD)] = (acc / total).astype(jnp.bfloat16)
        return 0

    lax.fori_loop(0, heads * blocks, one, 0)

def attend(seq, q, first, second, group=8):
    rows = second.shape[0]
    return pl.pallas_call(
        functools.partial(attend_kernel, group),
        out_shape=jax.ShapeDtypeStruct(q.shape, jnp.bfloat16),
        in_specs=[pl.BlockSpec(memory_space=pltpu.SMEM)]+[pl.BlockSpec(memory_space=pltpu.VMEM)]*3,
        out_specs=pl.BlockSpec(memory_space=pltpu.VMEM),
        scratch_shapes=[pltpu.VMEM((rows, HEAD), jnp.float32), pltpu.VMEM((rows, HEAD), jnp.float32),
            pltpu.VMEM((5*BLK, HEAD), jnp.bfloat16), pltpu.VMEM((5*BLK, HEAD), jnp.bfloat16),
            pltpu.VMEM((WIN2, BLK, 4*BLK), jnp.float32), pltpu.VMEM((4, BLK, BLK), jnp.float32), pltpu.VMEM((4, BLK, BLK), jnp.float32)],
        compiler_params=pltpu.CompilerParams(vmem_limit_bytes=40*1024*1024),
    )(seq, q, first, second)


def swap_rows(value):
    return lax.ppermute(value, "head", [(i, (i + 8) % 16) for i in range(16)])


def along_z(value, step):
    return lax.ppermute(
        value, "head", [(i, (i // 8) * 8 + (i + step) % 8) for i in range(16)]
    )


def along_seq(value, step):
    return lax.ppermute(value, "seq", [(i, i + step) for i in range(16 - step)])


def round_x(value, step):
    return lax.ppermute(value, "seq", [(i, (i + 4 * step) % 16) for i in range(16)])


def other_core(value):
    return lax.ppermute(value, "seq", [(i, i ^ 1) for i in range(16)])


def ring_sum(mine, add):
    other = swap_rows(mine)
    total = add(None, 0, mine, other)
    pair = jnp.concatenate([mine[None], other[None]], axis=0)
    up = down = pair
    for step in range(1, 5):
        up = along_z(up, 1)
        if step < 4:
            down = along_z(down, -1)
        total = add(total, -step, up[0], up[1])
        if step < 4:
            total = add(total, step, down[0], down[1])
    return total


def sent_to_all(value, axis):
    size = lax.axis_size(axis)
    return lax.all_to_all(
        jnp.broadcast_to(value[None], (size, *value.shape)), axis, 0, 0, tiled=True
    )


def owned_columns(w_out):
    seq = lax.axis_index("seq")
    x, core = seq >> 2, seq & 1
    rows, width = w_out.shape
    part = rows // 8
    piece = lax.dynamic_slice_in_dim(w_out, (2 * x + core) * part, part, 0)
    piece = piece.reshape(part, 16, width // 16).transpose(1, 0, 2)
    piece = lax.all_to_all(piece, "head", 0, 0, tiled=True)
    held = jnp.zeros((4, *piece.shape), piece.dtype)
    held = lax.dynamic_update_slice_in_dim(held, piece[None], x, 0)
    for step in (1, 3, 2):
        moved = round_x(piece, step)
        held = lax.dynamic_update_slice_in_dim(held, moved[None], (x - step) & 3, 0)
    twin = other_core(held)
    first = jnp.where(core == 0, held, twin)
    second = jnp.where(core == 0, twin, held)
    both = jnp.stack([first, second], axis=0)
    return both.transpose(2, 1, 0, 3, 4).reshape(rows * 16, width // 16)


def body(tokens, w_query, w_keyval, w_out):
    tok_rows, depth = tokens.shape
    head = lax.axis_index("head")
    far_row = (head & 8) ^ 8

    def places(offset):
        spot = (head + offset) & 7
        return (head & 8) | spot, far_row | spot

    def rows_of(matrix, place, count):
        return lax.dynamic_slice_in_dim(matrix, place * count, count, 0)

    def dot(a, b):
        return jnp.dot(a, b, preferred_element_type=jnp.float32)

    def project(total, offset, mine, other):
        near, far = places(offset)
        new = [
            dot(mine, rows_of(w, near, depth)) + dot(other, rows_of(w, far, depth))
            for w in (w_query, w_keyval)
        ]
        return new if total is None else [a + b for a, b in zip(total, new)]

    query_sum, keyval_sum = ring_sum(tokens, project)
    queries = query_sum.astype(jnp.bfloat16)
    own = keyval_sum.astype(jnp.bfloat16)
    keyval = sent_to_all(own, "head").transpose(1, 0, 2).reshape(tok_rows, 4 * HEAD)
    first_pair = keyval[:, : 2 * HEAD]
    second_pair = keyval[:, 2 * HEAD :]
    near_first = along_seq(first_pair, 1)
    near_tail = along_seq(second_pair[tok_rows - WIN2 :], 1)
    far_first = along_seq(first_pair, 2)
    first_ext = jnp.concatenate([far_first, near_first, first_pair], axis=0)
    second_ext = jnp.concatenate([near_tail, second_pair], axis=0)
    seq = lax.axis_index("seq").astype(jnp.int32).reshape(1)
    attended = attend(seq, queries, first_ext, second_ext)
    columns = owned_columns(w_out)
    feats = attended.shape[1]

    def finish(total, offset, mine, other):
        near, far = places(offset)
        new = dot(mine, rows_of(columns, near, feats)) + dot(other, rows_of(columns, far, feats))
        return new if total is None else total + new

    return ring_sum(attended, finish).astype(jnp.bfloat16)


def solution(mesh):
    return jax.shard_map(
        body,
        mesh=mesh,
        in_specs=(P("seq", "head"), P(None, "head"), P(None, "head"), P("head", None)),
        out_specs=P("seq", "head"),
        check_vma=False,
    )
```

```python
import jax
import jax.numpy as jnp
from jax import lax
from jax.experimental import pallas as pl
from jax.experimental.pallas import tpu as pltpu
from jax.sharding import PartitionSpec as P


HEAD = 128
WIN1 = 512
WIN2 = 32
BLK = 128
GROUP = 8
LOW = -1e30
LANES = (((1,), (1,)), ((), ()))


def attend_kernel(
    seq_ref, mine_ref, sent_ref, far_ref, near_ref, own_ref, out_ref,
    k2f, v2f, ktile, vtile, kpair, vpair, s_scr, mx_scr, mcb_scr,
):
    tok = mine_ref.shape[0]
    heads = mine_ref.shape[1] // HEAD
    blocks = tok // BLK
    seq = seq_ref[0]
    coef = (HEAD ** -0.5) * 1.4426950408889634
    start = seq == 0

    for t in range(6):
        source = (far_ref, near_ref, own_ref)[t // 2]
        lanes = slice((t % 2) * BLK, (t % 2 + 1) * BLK)
        ktile[t] = source[:HEAD, lanes]
        vtile[t] = source[HEAD:2 * HEAD, lanes].astype(jnp.float32).T.astype(jnp.bfloat16)
    for scr, low in ((k2f, 2 * HEAD), (v2f, 3 * HEAD)):
        scr[:BLK] = near_ref[low:low + HEAD, tok - BLK:].astype(jnp.float32).T
        for t in range(blocks):
            scr[(t + 1) * BLK:(t + 2) * BLK] = own_ref[low:low + HEAD, t * BLK:(t + 1) * BLK].astype(jnp.float32).T

    @pl.when(start)
    def _():
        k2f[:BLK] = jnp.broadcast_to(k2f[BLK:BLK + 1], (BLK, HEAD))
        v2f[:BLK] = jnp.zeros((BLK, HEAD), jnp.float32)

    row = lax.broadcasted_iota(jnp.int32, (BLK, BLK), 0)
    col = lax.broadcasted_iota(jnp.int32, (BLK, BLK), 1)
    early = col > row
    absent = jnp.maximum(WIN1 - seq * tok, 0) // BLK

    def one(combo, _):
        h = combo // blocks
        b = combo % blocks
        base = pl.multiple_of(b * BLK, BLK)
        hcol = pl.multiple_of(h * HEAD, HEAD)
        at = (pl.ds(base, BLK), pl.ds(hcol, HEAD))
        qf = (mine_ref[at] + sent_ref[at]).astype(jnp.bfloat16).astype(jnp.float32)
        for slot, t in enumerate((0, 4, 1, 2, 3)):
            kpair[:, slot * BLK:(slot + 1) * BLK] = ktile[b + t]
            vpair[slot * BLK:(slot + 1) * BLK] = vtile[b + t]
        mx_scr[...] = jnp.full(mx_scr.shape, LOW, jnp.float32)

        def scores(step, _):
            lag0 = step * GROUP
            prods = []
            for g in range(GROUP):
                k2 = k2f[pl.ds(BLK + base - lag0 - g, BLK), :]
                prods.append((qf * k2).astype(jnp.bfloat16))
            prod = jnp.concatenate(prods, axis=0)
            for t in range(3):
                width = 2 * BLK if t < 2 else BLK
                s = jnp.dot(prod, kpair[:, 2 * BLK * t:2 * BLK * t + width], preferred_element_type=jnp.float32)
                s = s.reshape(GROUP, BLK, width)
                if t == 0:
                    parts = [(0, jnp.where(early[None], s[:, :, :BLK], s[:, :, BLK:]))]
                elif t == 1:
                    parts = [(1, s[:, :, :BLK]), (2, s[:, :, BLK:])]
                else:
                    parts = [(3, s)]
                for place, value in parts:
                    s_scr[pl.ds(lag0, GROUP), :, place * BLK:(place + 1) * BLK] = value
                    top = value[0]
                    for g in range(1, GROUP):
                        top = jnp.maximum(top, value[g])
                    mx_scr[place] = jnp.maximum(mx_scr[place], top)
            return 0

        lax.fori_loop(0, WIN2 // GROUP, scores, 0)
        tops = []
        gone = []
        for place in range(4):
            hide = (b + place) < absent
            mask = early if place == 0 else row >= 0
            gone.append(jnp.logical_and(mask, hide))
            tops.append(jnp.where(gone[place], LOW, mx_scr[place]))
        top = jnp.maximum(jnp.maximum(tops[0], tops[1]), jnp.maximum(tops[2], tops[3]))
        peak = jnp.max(top, axis=1, keepdims=True) * coef
        for place in range(4):
            mcb_scr[place] = jnp.where(gone[place], -LOW, jnp.broadcast_to(peak, (BLK, BLK)))

        def raised_at(lag):
            return [
                jnp.exp2(s_scr[lag, :, p * BLK:(p + 1) * BLK] * coef - mcb_scr[p])
                for p in range(4)
            ]

        def mix(lag, carry):
            acc, tot = carry
            raised = raised_at(lag)
            tot = tot + ((raised[0] + raised[1]) + (raised[2] + raised[3]))
            split = [jnp.where(early, raised[0], 0.0), jnp.where(early, 0.0, raised[0])]
            w = jnp.concatenate([part.astype(jnp.bfloat16) for part in split + raised[1:]], axis=1)
            m = jnp.dot(w, vpair[...], preferred_element_type=jnp.float32)
            acc = acc + m * v2f[pl.ds(BLK + base - lag, BLK), :]
            return acc, tot

        zero = jnp.zeros((BLK, HEAD), jnp.float32)
        acc, tot = lax.fori_loop(0, WIN2, mix, (zero, zero), unroll=4)
        last = raised_at(WIN2 - 1)
        spare = jnp.where(jnp.logical_and(start, b == 0), jnp.maximum(WIN2 - 1 - row, 0), 0)
        tot = tot - spare.astype(jnp.float32) * ((last[0] + last[1]) + (last[2] + last[3]))
        total = jnp.sum(tot, axis=1, keepdims=True)
        out_ref[at] = (acc / total).astype(jnp.bfloat16)
        return 0

    lax.fori_loop(0, heads * blocks, one, 0)


def in_vmem(count):
    return [pl.BlockSpec(memory_space=pltpu.VMEM)] * count


def attend(seq, mine, sent, far, near, own):
    tok = mine.shape[0]
    return pl.pallas_call(
        attend_kernel,
        out_shape=jax.ShapeDtypeStruct(mine.shape, jnp.bfloat16),
        in_specs=[pl.BlockSpec(memory_space=pltpu.SMEM)] + in_vmem(5),
        out_specs=in_vmem(1)[0],
        scratch_shapes=[
            pltpu.VMEM((BLK + tok, HEAD), jnp.float32),
            pltpu.VMEM((BLK + tok, HEAD), jnp.float32),
            pltpu.VMEM((6, HEAD, BLK), jnp.bfloat16),
            pltpu.VMEM((6, BLK, HEAD), jnp.bfloat16),
            pltpu.VMEM((HEAD, 5 * BLK), jnp.bfloat16),
            pltpu.VMEM((5 * BLK, HEAD), jnp.bfloat16),
            pltpu.VMEM((WIN2, BLK, 4 * BLK), jnp.float32),
            pltpu.VMEM((4, BLK, BLK), jnp.float32),
            pltpu.VMEM((4, BLK, BLK), jnp.float32),
        ],
        compiler_params=pltpu.CompilerParams(vmem_limit_bytes=24 * 1024 * 1024),
    )(seq, mine, sent, far, near, own)


OFFSETS = (0, -1, 1, -2, 2, -3, 3, -4)


def project_kernel(spot_ref, *refs):
    shards, kv_own, kv_part, own_ref, same_ref, twin_ref = refs[:8], *refs[8:13]
    kv_mine, kv_theirs, mine_out, theirs_out = refs[13:]
    depth = shards[0].shape[1]
    core = spot_ref[1]

    def from_place(offset, count):
        spot = (spot_ref[0] + offset) & (count - 1)
        return pl.ds(pl.multiple_of(spot * depth, depth), depth)

    for weight, out in ((kv_own, kv_mine), (kv_part, kv_theirs)):
        total = None
        for offset, shard in zip(OFFSETS, shards):
            cols = weight[:, from_place(offset, 8)]
            new = lax.dot_general(cols, shard[...], LANES, preferred_element_type=jnp.float32)
            total = new if total is None else total + new
        out[...] = total
    total = None
    for offset, shard in zip(OFFSETS, shards):
        new = jnp.dot(shard[...], own_ref[from_place(offset, 8), :], preferred_element_type=jnp.float32)
        total = new if total is None else total + new
    mine_out[...] = total
    theirs_out[...] = jnp.zeros(theirs_out.shape, jnp.float32)
    for offset, shard in zip(OFFSETS, shards):
        low = from_place(offset, 4)
        upper = ((spot_ref[0] + offset) & 7) >> 2
        for ref, side in ((same_ref, core), (twin_ref, 1 - core)):

            @pl.when(upper == side)
            def _():
                theirs_out[...] += jnp.dot(shard[...], ref[low, :], preferred_element_type=jnp.float32)


def project(spots, arrays, shapes):
    return pl.pallas_call(
        project_kernel,
        out_shape=tuple(jax.ShapeDtypeStruct(shape, jnp.float32) for shape in shapes),
        in_specs=[pl.BlockSpec(memory_space=pltpu.SMEM)] + in_vmem(len(arrays)),
        out_specs=tuple(in_vmem(len(shapes))),
        compiler_params=pltpu.CompilerParams(vmem_limit_bytes=24 * 1024 * 1024),
    )(spots, *arrays)


def swap_rows(value):
    return lax.ppermute(value, "head", [(i, (i + 8) % 16) for i in range(16)])


def along_z(value, step):
    return lax.ppermute(
        value, "head", [(i, (i // 8) * 8 + (i + step) % 8) for i in range(16)]
    )


def along_seq(value, step):
    return lax.ppermute(value, "seq", [(i, i + step) for i in range(16 - step)])


def round_x(value, step):
    return lax.ppermute(value, "seq", [(i, (i + 4 * step) % 16) for i in range(16)])


def other_core(value):
    return lax.ppermute(value, "seq", [(i, i ^ 1) for i in range(16)])


def z_ring(value):
    found = [value]
    up = down = value
    for step in range(1, 5):
        up = along_z(up, 1)
        if step < 4:
            down = along_z(down, -1)
        if step < 4:
            up, down = lax.optimization_barrier((up, down))
            found += [up, down]
        else:
            found.append(up)
    return found


def sent_to_all(value, axis):
    size = lax.axis_size(axis)
    return lax.all_to_all(
        jnp.broadcast_to(value[None], (size, *value.shape)), axis, 0, 0, tiled=True
    )


def owned_piece(w_out, seq):
    x, core = seq >> 2, seq & 1
    rows, width = w_out.shape
    part = rows // 8
    piece = lax.dynamic_slice_in_dim(w_out, (2 * x + core) * part, part, 0)
    return piece.reshape(part, 16, width // 16).transpose(1, 0, 2)


def owned_columns(piece, seq):
    x = seq >> 2
    piece = lax.all_to_all(piece, "head", 0, 0, tiled=True)
    held = jnp.zeros((4, *piece.shape), piece.dtype)
    held = lax.dynamic_update_slice_in_dim(held, piece[None], x, 0)
    for step in (1, 3, 2):
        moved = round_x(piece, step)
        held = lax.dynamic_update_slice_in_dim(held, moved[None], (x - step) & 3, 0)
    return held, other_core(held)


def gather_rows(spot_ref, held, twin, place, out, slot):
    core = spot_ref[1]
    part = held.shape[2]
    for x in range(4):
        for source, side in ((held, core), (twin, 1 - core)):
            low = pl.multiple_of(x * 2 * part + side * part, part)
            out[slot, pl.ds(low, part), :] = source[x, place]


def finish_kernel(spot_ref, *refs):
    near, far, pairs, held, twin = refs[0], refs[1], refs[2:8], refs[8], refs[9]
    part_out, tail_out, w_scr = refs[10:]
    total = None
    values = [(near, far)] + [(pair.at[0], pair.at[1]) for pair in pairs]
    for k, offset in enumerate(OFFSETS):
        spot = (spot_ref[0] + offset) & 7
        for side in range(2):
            place = ((spot_ref[0] & 8) ^ (8 * side)) | spot
            if k == 7:
                gather_rows(spot_ref, held, twin, place, tail_out, side)
                continue
            gather_rows(spot_ref, held, twin, place, w_scr, 2 * k + side)
            new = jnp.dot(values[k][side][...], w_scr[2 * k + side], preferred_element_type=jnp.float32)
            total = new if total is None else total + new
    part_out[...] = total


def close_kernel(part_ref, tail_ref, pair_ref, out_ref):
    total = part_ref[...]
    for side in range(2):
        total = total + jnp.dot(pair_ref[side], tail_ref[side], preferred_element_type=jnp.float32)
    out_ref[...] = total.astype(jnp.bfloat16)


def finish(spots, near, pairs, held, twin):
    tok, feats = near.shape
    cols = held.shape[-1]
    limit = pltpu.CompilerParams(vmem_limit_bytes=24 * 1024 * 1024)
    part, tail = pl.pallas_call(
        finish_kernel,
        out_shape=(
            jax.ShapeDtypeStruct((tok, cols), jnp.float32),
            jax.ShapeDtypeStruct((2, feats, cols), held.dtype),
        ),
        in_specs=[pl.BlockSpec(memory_space=pltpu.SMEM)] + in_vmem(10),
        out_specs=tuple(in_vmem(2)),
        scratch_shapes=[pltpu.VMEM((14, feats, cols), held.dtype)],
        compiler_params=limit,
    )(spots, *near_and(near, pairs), held, twin)
    return pl.pallas_call(
        close_kernel,
        out_shape=jax.ShapeDtypeStruct((tok, cols), jnp.bfloat16),
        in_specs=in_vmem(3),
        out_specs=in_vmem(1)[0],
        compiler_params=limit,
    )(part, tail, pairs[7])


def near_and(near, pairs):
    return (near, pairs[0][1], *pairs[1:7])


def body(tokens, w_query, w_keyval, w_out):
    tok_rows = tokens.shape[0]
    head = lax.axis_index("head").astype(jnp.int32)
    seq = lax.axis_index("seq").astype(jnp.int32)
    row, core = head >> 3, seq & 1
    spots = jnp.stack([head, core])
    half = w_query.shape[0] // 2
    quarter = half // 2
    kv_flat = w_keyval.T
    kv_part = swap_rows(lax.dynamic_slice_in_dim(kv_flat, (1 - row) * half, half, 1))
    q_same = swap_rows(
        lax.dynamic_slice_in_dim(w_query, (1 - row) * half + core * quarter, quarter, 0)
    )
    q_twin = other_core(q_same)
    kv_own = lax.dynamic_slice_in_dim(kv_flat, row * half, half, 1)
    q_own = lax.dynamic_slice_in_dim(w_query, row * half, half, 0)
    shards = z_ring(tokens)
    piece, shards[5], shards[6] = lax.optimization_barrier(
        (owned_piece(w_out, seq), shards[5], shards[6])
    )
    kv_mine, kv_theirs, q_mine, q_theirs = project(
        spots,
        (*shards, kv_own, kv_part, q_own, q_same, q_twin),
        ((kv_flat.shape[0], tok_rows),) * 2 + ((tok_rows, w_query.shape[1]),) * 2,
    )
    kv = (kv_mine + swap_rows(kv_theirs)).astype(jnp.bfloat16)
    q_sent = swap_rows(q_theirs)
    keyval = sent_to_all(kv, "head").reshape(4 * HEAD, tok_rows)
    near = along_seq(keyval, 1)
    far = along_seq(keyval[:2 * HEAD], 2)
    attended = attend(seq.reshape(1), q_mine, q_sent, far, near, keyval)
    held, twin = owned_columns(piece, seq)
    other = swap_rows(attended)
    pairs = z_ring(jnp.concatenate([attended[None], other[None]], axis=0))
    pairs[0] = (attended, other)
    return finish(spots, attended, pairs, held, twin)


def solution(mesh):
    return jax.shard_map(
        body,
        mesh=mesh,
        in_specs=(P("seq", "head"), P(None, "head"), P(None, "head"), P("head", None)),
        out_specs=P("seq", "head"),
        check_vma=False,
    )
```

```python
import jax
import jax.numpy as jnp
from jax import lax
from jax.experimental import pallas as pl
from jax.experimental.pallas import tpu as pltpu
from jax.sharding import PartitionSpec as P


HEAD = 128
WIN1 = 512
WIN2 = 32
BLK = 128
GROUP = 8
LOW = -1e30
LANES = (((1,), (1,)), ((), ()))


def pick(source, which, lanes):
    places = slice((which % 2) * 4, (which % 2) * 4 + 4)
    found = source[places, :, lanes] if len(source.shape) == 3 else source[places, which // 2, :, lanes]
    return found.reshape(HEAD, BLK)


def attend_kernel(
    seq_ref, mine_ref, sent_ref, far_ref, near_ref, own_ref, out_ref,
    k2f, v2f, ktile, vtile, kpair, vpair, s_scr, mx_scr, mcb_scr,
):
    tok = mine_ref.shape[0]
    heads = mine_ref.shape[1] // HEAD
    blocks = tok // BLK
    seq = seq_ref[0]
    coef = (HEAD ** -0.5) * 1.4426950408889634
    start = seq == 0

    for t in range(6):
        source = (far_ref, near_ref, own_ref)[t // 2]
        lanes = slice((t % 2) * BLK, (t % 2 + 1) * BLK)
        ktile[t] = pick(source, 0, lanes)
        vtile[t] = pick(source, 1, lanes).astype(jnp.float32).T.astype(jnp.bfloat16)
    for scr, which in ((k2f, 2), (v2f, 3)):
        scr[:BLK] = pick(near_ref, which, slice(tok - BLK, tok)).astype(jnp.float32).T
        for t in range(blocks):
            scr[(t + 1) * BLK:(t + 2) * BLK] = pick(own_ref, which, slice(t * BLK, (t + 1) * BLK)).astype(jnp.float32).T

    @pl.when(start)
    def _():
        k2f[:BLK] = jnp.broadcast_to(k2f[BLK:BLK + 1], (BLK, HEAD))
        v2f[:BLK] = jnp.zeros((BLK, HEAD), jnp.float32)

    row = lax.broadcasted_iota(jnp.int32, (BLK, BLK), 0)
    col = lax.broadcasted_iota(jnp.int32, (BLK, BLK), 1)
    early = col > row
    absent = jnp.maximum(WIN1 - seq * tok, 0) // BLK

    def one(combo, _):
        h = combo // blocks
        b = combo % blocks
        base = pl.multiple_of(b * BLK, BLK)
        hcol = pl.multiple_of(h * HEAD, HEAD)
        at = (pl.ds(base, BLK), pl.ds(hcol, HEAD))
        qf = (mine_ref[at] + sent_ref[at]).astype(jnp.bfloat16).astype(jnp.float32)
        for slot, t in enumerate((0, 4, 1, 2, 3)):
            kpair[:, slot * BLK:(slot + 1) * BLK] = ktile[b + t]
            vpair[slot * BLK:(slot + 1) * BLK] = vtile[b + t]
        mx_scr[...] = jnp.full(mx_scr.shape, LOW, jnp.float32)

        def scores(step, _):
            lag0 = step * GROUP
            prods = []
            for g in range(GROUP):
                k2 = k2f[pl.ds(BLK + base - lag0 - g, BLK), :]
                prods.append((qf * k2).astype(jnp.bfloat16))
            prod = jnp.concatenate(prods, axis=0)
            for t in range(3):
                width = 2 * BLK if t < 2 else BLK
                s = jnp.dot(prod, kpair[:, 2 * BLK * t:2 * BLK * t + width], preferred_element_type=jnp.float32)
                s = s.reshape(GROUP, BLK, width)
                if t == 0:
                    parts = [(0, jnp.where(early[None], s[:, :, :BLK], s[:, :, BLK:]))]
                elif t == 1:
                    parts = [(1, s[:, :, :BLK]), (2, s[:, :, BLK:])]
                else:
                    parts = [(3, s)]
                for place, value in parts:
                    s_scr[pl.ds(lag0, GROUP), :, place * BLK:(place + 1) * BLK] = value
                    top = value[0]
                    for g in range(1, GROUP):
                        top = jnp.maximum(top, value[g])
                    mx_scr[place] = jnp.maximum(mx_scr[place], top)
            return 0

        lax.fori_loop(0, WIN2 // GROUP, scores, 0)
        tops = []
        gone = []
        for place in range(4):
            hide = (b + place) < absent
            mask = early if place == 0 else row >= 0
            gone.append(jnp.logical_and(mask, hide))
            tops.append(jnp.where(gone[place], LOW, mx_scr[place]))
        top = jnp.maximum(jnp.maximum(tops[0], tops[1]), jnp.maximum(tops[2], tops[3]))
        peak = jnp.max(top, axis=1, keepdims=True) * coef
        for place in range(4):
            mcb_scr[place] = jnp.where(gone[place], -LOW, jnp.broadcast_to(peak, (BLK, BLK)))

        def raised_at(lag):
            return [
                jnp.exp2(s_scr[lag, :, p * BLK:(p + 1) * BLK] * coef - mcb_scr[p])
                for p in range(4)
            ]

        def mix(lag, carry):
            acc, tot = carry
            raised = raised_at(lag)
            tot = tot + ((raised[0] + raised[1]) + (raised[2] + raised[3]))
            split = [jnp.where(early, raised[0], 0.0), jnp.where(early, 0.0, raised[0])]
            w = jnp.concatenate([part.astype(jnp.bfloat16) for part in split + raised[1:]], axis=1)
            m = jnp.dot(w, vpair[...], preferred_element_type=jnp.float32)
            acc = acc + m * v2f[pl.ds(BLK + base - lag, BLK), :]
            return acc, tot

        zero = jnp.zeros((BLK, HEAD), jnp.float32)
        acc, tot = lax.fori_loop(0, WIN2, mix, (zero, zero), unroll=4)
        last = raised_at(WIN2 - 1)
        spare = jnp.where(jnp.logical_and(start, b == 0), jnp.maximum(WIN2 - 1 - row, 0), 0)
        tot = tot - spare.astype(jnp.float32) * ((last[0] + last[1]) + (last[2] + last[3]))
        total = jnp.sum(tot, axis=1, keepdims=True)
        out_ref[at] = (acc / total).astype(jnp.bfloat16)
        return 0

    lax.fori_loop(0, heads * blocks, one, 0)


def in_vmem(count):
    return [pl.BlockSpec(memory_space=pltpu.VMEM)] * count


def attend(seq, mine, sent, far, near, own):
    tok = mine.shape[0]
    return pl.pallas_call(
        attend_kernel,
        out_shape=jax.ShapeDtypeStruct(mine.shape, jnp.bfloat16),
        in_specs=[pl.BlockSpec(memory_space=pltpu.SMEM)] + in_vmem(5),
        out_specs=in_vmem(1)[0],
        scratch_shapes=[
            pltpu.VMEM((BLK + tok, HEAD), jnp.float32),
            pltpu.VMEM((BLK + tok, HEAD), jnp.float32),
            pltpu.VMEM((6, HEAD, BLK), jnp.bfloat16),
            pltpu.VMEM((6, BLK, HEAD), jnp.bfloat16),
            pltpu.VMEM((HEAD, 5 * BLK), jnp.bfloat16),
            pltpu.VMEM((5 * BLK, HEAD), jnp.bfloat16),
            pltpu.VMEM((WIN2, BLK, 4 * BLK), jnp.float32),
            pltpu.VMEM((4, BLK, BLK), jnp.float32),
            pltpu.VMEM((4, BLK, BLK), jnp.float32),
        ],
        compiler_params=pltpu.CompilerParams(vmem_limit_bytes=24 * 1024 * 1024),
    )(seq, mine, sent, far, near, own)


OFFSETS = (0, -1, 1, -2, 2, -3, 3, -4)


def project_kernel(spot_ref, *refs):
    shards, kv_own, kv_part, own_any, same_ref, twin_ref = refs[:8], *refs[8:13]
    kv_out, mine_out, theirs_out, own_ref, sem = refs[13:]
    depth = shards[0].shape[1]
    half = own_ref.shape[0]
    row, core = spot_ref[0] >> 3, spot_ref[1]
    fetch = pltpu.make_async_copy(
        own_any.at[pl.ds(pl.multiple_of(row * half, half), half), :], own_ref, sem
    )
    fetch.start()

    def from_place(offset, count):
        spot = (spot_ref[0] + offset) & (count - 1)
        return pl.ds(pl.multiple_of(spot * depth, depth), depth)

    parts = kv_own.shape[0]
    for weight, side in ((kv_own, row), (kv_part, 1 - row)):
        total = None
        for offset, shard in zip(OFFSETS, shards):
            cols = weight[:, from_place(offset, 8)]
            new = lax.dot_general(cols, shard[...], LANES, preferred_element_type=jnp.float32)
            total = new if total is None else total + new
        kv_out[pl.ds(pl.multiple_of(side * parts, parts), parts), :] = total
    theirs_out[...] = jnp.zeros(theirs_out.shape, jnp.float32)
    for offset, shard in zip(OFFSETS, shards):
        low = from_place(offset, 4)
        upper = ((spot_ref[0] + offset) & 7) >> 2
        for ref, side in ((same_ref, core), (twin_ref, 1 - core)):

            @pl.when(upper == side)
            def _():
                theirs_out[...] += jnp.dot(shard[...], ref[low, :], preferred_element_type=jnp.float32)
    fetch.wait()
    total = None
    for offset, shard in zip(OFFSETS, shards):
        new = jnp.dot(shard[...], own_ref[from_place(offset, 8), :], preferred_element_type=jnp.float32)
        total = new if total is None else total + new
    mine_out[...] = total


def project(spots, arrays, shapes):
    specs = in_vmem(len(arrays))
    specs[10] = pl.BlockSpec(memory_space=pl.ANY)
    own = arrays[10]
    return pl.pallas_call(
        project_kernel,
        out_shape=tuple(jax.ShapeDtypeStruct(shape, jnp.float32) for shape in shapes),
        in_specs=[pl.BlockSpec(memory_space=pltpu.SMEM)] + specs,
        out_specs=tuple(in_vmem(len(shapes))),
        scratch_shapes=[
            pltpu.VMEM((own.shape[0] // 2, own.shape[1]), own.dtype),
            pltpu.SemaphoreType.DMA,
        ],
        compiler_params=pltpu.CompilerParams(vmem_limit_bytes=24 * 1024 * 1024),
    )(spots, *arrays)


def swap_rows(value):
    return lax.ppermute(value, "head", [(i, (i + 8) % 16) for i in range(16)])


def along_z(value, step):
    return lax.ppermute(
        value, "head", [(i, (i // 8) * 8 + (i + step) % 8) for i in range(16)]
    )


def along_seq(value, step):
    return lax.ppermute(value, "seq", [(i, i + step) for i in range(16 - step)])


def round_x(value, step):
    return lax.ppermute(value, "seq", [(i, (i + 4 * step) % 16) for i in range(16)])


def other_core(value):
    return lax.ppermute(value, "seq", [(i, i ^ 1) for i in range(16)])


def z_ring(value):
    found = [value]
    up = down = value
    for step in range(1, 5):
        up = along_z(up, 1)
        if step < 4:
            down = along_z(down, -1)
        if step < 4:
            up, down = lax.optimization_barrier((up, down))
            found += [up, down]
        else:
            found.append(up)
    return found


ROWS = [list(range(8)), list(range(8, 16))]


def sent_to_row(value):
    return lax.all_to_all(
        jnp.broadcast_to(value[None], (8, *value.shape)),
        "head", 0, 0, tiled=True, axis_index_groups=ROWS,
    )


def owned_piece(w_out, seq):
    x, core = seq >> 2, seq & 1
    rows, width = w_out.shape
    part = rows // 8
    piece = lax.dynamic_slice_in_dim(w_out, (2 * x + core) * part, part, 0)
    return piece.reshape(part, 16, width // 16).transpose(1, 0, 2)


def owned_columns(piece, seq, tie):
    x = seq >> 2
    moved = [round_x(piece, step) for step in (1, 3, 2)]
    *moved, tie = lax.optimization_barrier((*moved, tie))
    held = jnp.zeros((4, *piece.shape), piece.dtype)
    held = lax.dynamic_update_slice_in_dim(held, piece[None], x, 0)
    for step, part in zip((1, 3, 2), moved):
        held = lax.dynamic_update_slice_in_dim(held, part[None], (x - step) & 3, 0)
    return held, other_core(held), tie


def two_rings(value):
    other = swap_rows(value)
    rings = []
    for start in (value, other):
        rings.append(z_ring(start))
    return rings


def gather_rows(spot_ref, held, twin, place, out, slot):
    core = spot_ref[1]
    part = held.shape[2]
    for x in range(4):
        for source, side in ((held, core), (twin, 1 - core)):
            low = pl.multiple_of(x * 2 * part + side * part, part)
            out[slot, pl.ds(low, part), :] = source[x, place]


def finish_kernel(spot_ref, *refs):
    mine, other, held, twin = refs[:8], refs[8:15], refs[15], refs[16]
    part_out, tail_out, w_scr = refs[17:]
    total = None
    for side, values in enumerate((mine, other)):
        for k, value in enumerate(values):
            place = ((spot_ref[0] & 8) ^ (8 * side)) | ((spot_ref[0] + OFFSETS[k]) & 7)
            slot = 8 * side + k
            gather_rows(spot_ref, held, twin, place, w_scr, slot)
            new = jnp.dot(value[...], w_scr[slot], preferred_element_type=jnp.float32)
            total = new if total is None else total + new
    part_out[...] = total
    place = ((spot_ref[0] & 8) ^ 8) | ((spot_ref[0] + OFFSETS[7]) & 7)
    gather_rows(spot_ref, held, twin, place, tail_out, 0)


def close_kernel(part_ref, tail_ref, last_ref, out_ref):
    total = part_ref[...] + jnp.dot(last_ref[...], tail_ref[0], preferred_element_type=jnp.float32)
    out_ref[...] = total.astype(jnp.bfloat16)


def finish(spots, mine, other, held, twin):
    tok, feats = mine[0].shape
    cols = held.shape[-1]
    limit = pltpu.CompilerParams(vmem_limit_bytes=24 * 1024 * 1024)
    part, tail = pl.pallas_call(
        finish_kernel,
        out_shape=(
            jax.ShapeDtypeStruct((tok, cols), jnp.float32),
            jax.ShapeDtypeStruct((1, feats, cols), held.dtype),
        ),
        in_specs=[pl.BlockSpec(memory_space=pltpu.SMEM)] + in_vmem(17),
        out_specs=tuple(in_vmem(2)),
        scratch_shapes=[pltpu.VMEM((15, feats, cols), held.dtype)],
        compiler_params=limit,
    )(spots, *mine, *other[:7], held, twin)
    return pl.pallas_call(
        close_kernel,
        out_shape=jax.ShapeDtypeStruct((tok, cols), jnp.bfloat16),
        in_specs=in_vmem(3),
        out_specs=in_vmem(1)[0],
        compiler_params=limit,
    )(part, tail, other[7])


def body(tokens, w_query, w_keyval, w_out):
    tok_rows = tokens.shape[0]
    head = lax.axis_index("head").astype(jnp.int32)
    seq = lax.axis_index("seq").astype(jnp.int32)
    row, core = head >> 3, seq & 1
    spots = jnp.stack([head, core])
    half = w_query.shape[0] // 2
    quarter = half // 2
    kv_flat = w_keyval.T
    kv_part = swap_rows(lax.dynamic_slice_in_dim(kv_flat, (1 - row) * half, half, 1))
    q_same = swap_rows(
        lax.dynamic_slice_in_dim(w_query, (1 - row) * half + core * quarter, quarter, 0)
    )
    q_twin = other_core(q_same)
    kv_own = lax.dynamic_slice_in_dim(kv_flat, row * half, half, 1)
    shards = z_ring(tokens)
    piece, shards[5], shards[6] = lax.optimization_barrier(
        (owned_piece(w_out, seq), shards[5], shards[6])
    )
    piece = lax.all_to_all(piece, "head", 0, 0, tiled=True)
    kv_part, q_mine, q_theirs = project(
        spots,
        (*shards, kv_own, kv_part, w_query, q_same, q_twin),
        ((2 * kv_flat.shape[0], tok_rows),) + ((tok_rows, w_query.shape[1]),) * 2,
    )
    kv = (kv_part + swap_rows(kv_part)).astype(jnp.bfloat16)
    piece, kv = lax.optimization_barrier((piece, kv))
    q_sent = swap_rows(q_theirs)
    keyval = sent_to_row(kv).reshape(8, 2, kv_flat.shape[0], tok_rows)
    near = along_seq(keyval, 1)
    far = along_seq(keyval[:, 0], 2)
    attended = attend(seq.reshape(1), q_mine, q_sent, far, near, keyval)
    mine, other = two_rings(attended)
    held, twin, mine[5] = owned_columns(piece, seq, mine[5])
    return finish(spots, mine, other, held, twin)


def solution(mesh):
    return jax.shard_map(
        body,
        mesh=mesh,
        in_specs=(P("seq", "head"), P(None, "head"), P(None, "head"), P("head", None)),
        out_specs=P("seq", "head"),
        check_vma=False,
    )
```

```python
import jax
import jax.numpy as jnp
from jax import lax
from jax.experimental import pallas as pl
from jax.experimental.pallas import tpu as pltpu
from jax.sharding import PartitionSpec as P


HEAD = 128
WIN1 = 512
WIN2 = 32
BLK = 128
GROUP = 16
MIX = 16
LOW = -1e30
LANES = (((1,), (1,)), ((), ()))


OWN, NEAR, FAR = 0, 2, 4


def pick(gathered, source, which, lanes):
    places = slice((which % 2) * 4, (which % 2) * 4 + 4)
    return gathered[places, source + which // 2, :, lanes].reshape(HEAD, BLK)


def attend_kernel(
    seq_ref, mine_any, sent_any, all_ref, out_ref,
    k2f, v2f, ktile, vtile, kpair, vpair, s_scr, mx_scr, mcb_scr, mine_ref, sent_ref, sems,
):
    fetches = [
        pltpu.make_async_copy(source, target, sems.at[k])
        for k, (source, target) in enumerate(((mine_any, mine_ref), (sent_any, sent_ref)))
    ]
    for fetch in fetches:
        fetch.start()
    tok = mine_ref.shape[0]
    heads = mine_ref.shape[1] // HEAD
    blocks = tok // BLK
    seq = seq_ref[0]
    coef = (HEAD ** -0.5) * 1.4426950408889634
    start = seq == 0

    for t in range(6):
        source = (FAR, NEAR, OWN)[t // 2]
        lanes = slice((t % 2) * BLK, (t % 2 + 1) * BLK)
        ktile[t] = pick(all_ref, source, 0, lanes)
        vtile[t] = pick(all_ref, source, 1, lanes).astype(jnp.float32).T.astype(jnp.bfloat16)
    for scr, which in ((k2f, 2), (v2f, 3)):
        scr[:BLK] = pick(all_ref, NEAR, which, slice(tok - BLK, tok)).astype(jnp.float32).T
        for t in range(blocks):
            scr[(t + 1) * BLK:(t + 2) * BLK] = pick(all_ref, OWN, which, slice(t * BLK, (t + 1) * BLK)).astype(jnp.float32).T

    @pl.when(start)
    def _():
        k2f[:BLK] = jnp.broadcast_to(k2f[BLK:BLK + 1], (BLK, HEAD))
        v2f[:BLK] = jnp.zeros((BLK, HEAD), jnp.float32)

    for fetch in fetches:
        fetch.wait()
    row = lax.broadcasted_iota(jnp.int32, (BLK, BLK), 0)
    col = lax.broadcasted_iota(jnp.int32, (BLK, BLK), 1)
    early = col > row
    absent = jnp.maximum(WIN1 - seq * tok, 0) // BLK

    def one(combo, _):
        h = combo // blocks
        b = combo % blocks
        base = pl.multiple_of(b * BLK, BLK)
        hcol = pl.multiple_of(h * HEAD, HEAD)
        at = (pl.ds(base, BLK), pl.ds(hcol, HEAD))
        qf = (mine_ref[at] + sent_ref[at]).astype(jnp.bfloat16).astype(jnp.float32)
        for slot, t in enumerate((0, 4, 1, 2, 3)):
            kpair[:, slot * BLK:(slot + 1) * BLK] = ktile[b + t]
            vpair[slot * BLK:(slot + 1) * BLK] = vtile[b + t]
        mx_scr[...] = jnp.full(mx_scr.shape, LOW, jnp.float32)

        def scores(step, _):
            lag0 = step * GROUP
            prods = []
            for g in range(GROUP):
                k2 = k2f[pl.ds(BLK + base - lag0 - g, BLK), :]
                prods.append((qf * k2).astype(jnp.bfloat16))
            prod = jnp.concatenate(prods, axis=0)
            for t in range(3):
                width = 2 * BLK if t < 2 else BLK
                s = jnp.dot(prod, kpair[:, 2 * BLK * t:2 * BLK * t + width], preferred_element_type=jnp.float32)
                s = s.reshape(GROUP, BLK, width)
                if t == 0:
                    parts = [(0, jnp.where(early[None], s[:, :, :BLK], s[:, :, BLK:]))]
                elif t == 1:
                    parts = [(1, s[:, :, :BLK]), (2, s[:, :, BLK:])]
                else:
                    parts = [(3, s)]
                for place, value in parts:
                    s_scr[pl.ds(lag0, GROUP), :, place * BLK:(place + 1) * BLK] = value
                    top = value[0]
                    for g in range(1, GROUP):
                        top = jnp.maximum(top, value[g])
                    mx_scr[place] = jnp.maximum(mx_scr[place], top)
            return 0

        lax.fori_loop(0, WIN2 // GROUP, scores, 0)
        tops = []
        gone = []
        for place in range(4):
            hide = (b + place) < absent
            mask = early if place == 0 else row >= 0
            gone.append(jnp.logical_and(mask, hide))
            tops.append(jnp.where(gone[place], LOW, mx_scr[place]))
        top = jnp.maximum(jnp.maximum(tops[0], tops[1]), jnp.maximum(tops[2], tops[3]))
        peak = jnp.max(top, axis=1, keepdims=True) * coef
        for place in range(4):
            mcb_scr[place] = jnp.where(gone[place], -LOW, jnp.broadcast_to(peak, (BLK, BLK)))

        def raised_at(lag):
            return [
                jnp.exp2(s_scr[lag, :, p * BLK:(p + 1) * BLK] * coef - mcb_scr[p])
                for p in range(4)
            ]

        def mix(step, carry):
            acc, tot = carry
            ws = []
            for g in range(MIX):
                raised = raised_at(step * MIX + g)
                tot = tot + ((raised[0] + raised[1]) + (raised[2] + raised[3]))
                split = [jnp.where(early, raised[0], 0.0), jnp.where(early, 0.0, raised[0])]
                ws.append(jnp.concatenate([part.astype(jnp.bfloat16) for part in split + raised[1:]], axis=1))
            m = jnp.dot(jnp.concatenate(ws, axis=0), vpair[...], preferred_element_type=jnp.float32)
            for g in range(MIX):
                acc = acc + m[g * BLK:(g + 1) * BLK] * v2f[pl.ds(BLK + base - step * MIX - g, BLK), :]
            return acc, tot

        zero = jnp.zeros((BLK, HEAD), jnp.float32)
        acc, tot = lax.fori_loop(0, WIN2 // MIX, mix, (zero, zero))
        last = raised_at(WIN2 - 1)
        spare = jnp.where(jnp.logical_and(start, b == 0), jnp.maximum(WIN2 - 1 - row, 0), 0)
        tot = tot - spare.astype(jnp.float32) * ((last[0] + last[1]) + (last[2] + last[3]))
        total = jnp.sum(tot, axis=1, keepdims=True)
        out_ref[at] = (acc / total).astype(jnp.bfloat16)
        return 0

    lax.fori_loop(0, heads * blocks, one, 0)


def in_vmem(count):
    return [pl.BlockSpec(memory_space=pltpu.VMEM)] * count


def attend(seq, mine, sent, gathered):
    tok = mine.shape[0]
    return pl.pallas_call(
        attend_kernel,
        out_shape=jax.ShapeDtypeStruct(mine.shape, jnp.bfloat16),
        in_specs=[pl.BlockSpec(memory_space=pltpu.SMEM)]
        + [pl.BlockSpec(memory_space=pltpu.HBM)] * 2
        + in_vmem(1),
        out_specs=in_vmem(1)[0],
        scratch_shapes=[
            pltpu.VMEM((BLK + tok, HEAD), jnp.float32),
            pltpu.VMEM((BLK + tok, HEAD), jnp.float32),
            pltpu.VMEM((6, HEAD, BLK), jnp.bfloat16),
            pltpu.VMEM((6, BLK, HEAD), jnp.bfloat16),
            pltpu.VMEM((HEAD, 5 * BLK), jnp.bfloat16),
            pltpu.VMEM((5 * BLK, HEAD), jnp.bfloat16),
            pltpu.VMEM((WIN2, BLK, 4 * BLK), jnp.float32),
            pltpu.VMEM((4, BLK, BLK), jnp.float32),
            pltpu.VMEM((4, BLK, BLK), jnp.float32),
            pltpu.VMEM(mine.shape, jnp.float32),
            pltpu.VMEM(mine.shape, jnp.float32),
            pltpu.SemaphoreType.DMA((2,)),
        ],
        compiler_params=pltpu.CompilerParams(vmem_limit_bytes=24 * 1024 * 1024),
    )(seq, mine, sent, gathered)


OFFSETS = (0, -1, 1, -2, 2, -3, 3, -4)
OWN_WEIGHTS = 10


def project_kernel(spot_ref, *refs):
    sources = refs[:13]
    kv_out, mine_any, theirs_any = refs[13:16]
    held = refs[16:29]
    mine_out, theirs_out, sems = refs[29:]
    shards, kv_own, kv_part, own_ref, same_ref, twin_ref = held[:8], *held[8:]
    depth = shards[0].shape[1]
    half = own_ref.shape[0]
    row, core = spot_ref[0] >> 3, spot_ref[1]
    fetches = []
    for k, (source, target) in enumerate(zip(sources, held)):
        if k == OWN_WEIGHTS:
            source = source.at[pl.ds(pl.multiple_of(row * half, half), half), :]
        fetches.append(pltpu.make_async_copy(source, target, sems.at[k]))
        fetches[k].start()

    def from_place(offset, count):
        spot = (spot_ref[0] + offset) & (count - 1)
        return pl.ds(pl.multiple_of(spot * depth, depth), depth)

    for k in range(OWN_WEIGHTS):
        fetches[k].wait()
    parts = kv_own.shape[0]
    for weight, side in ((kv_own, row), (kv_part, 1 - row)):
        total = None
        for offset, shard in zip(OFFSETS, shards):
            cols = weight[:, from_place(offset, 8)]
            new = lax.dot_general(cols, shard[...], LANES, preferred_element_type=jnp.float32)
            total = new if total is None else total + new
        kv_out[pl.ds(pl.multiple_of(side * parts, parts), parts), :] = total
    for k in range(OWN_WEIGHTS, len(held)):
        fetches[k].wait()
    theirs_out[...] = jnp.zeros(theirs_out.shape, jnp.float32)
    for offset, shard in zip(OFFSETS, shards):
        low = from_place(offset, 4)
        upper = ((spot_ref[0] + offset) & 7) >> 2
        for ref, side in ((same_ref, core), (twin_ref, 1 - core)):

            @pl.when(upper == side)
            def _():
                theirs_out[...] += jnp.dot(shard[...], ref[low, :], preferred_element_type=jnp.float32)
    send = pltpu.make_async_copy(theirs_out, theirs_any, sems.at[len(held)])
    send.start()
    total = None
    for offset, shard in zip(OFFSETS, shards):
        new = jnp.dot(shard[...], own_ref[from_place(offset, 8), :], preferred_element_type=jnp.float32)
        total = new if total is None else total + new
    mine_out[...] = total
    keep = pltpu.make_async_copy(mine_out, mine_any, sems.at[len(held) + 1])
    keep.start()
    send.wait()
    keep.wait()


def project(spots, arrays, shapes):
    far_off = pl.BlockSpec(memory_space=pltpu.HBM)
    own = arrays[OWN_WEIGHTS]
    kept = [array.shape for array in arrays]
    kept[OWN_WEIGHTS] = (own.shape[0] // 2, own.shape[1])
    return pl.pallas_call(
        project_kernel,
        out_shape=tuple(jax.ShapeDtypeStruct(shape, jnp.float32) for shape in shapes),
        in_specs=[pl.BlockSpec(memory_space=pltpu.SMEM)] + [far_off] * len(arrays),
        out_specs=(in_vmem(1)[0], far_off, far_off),
        scratch_shapes=[pltpu.VMEM(shape, own.dtype) for shape in kept]
        + [pltpu.VMEM(shape, jnp.float32) for shape in shapes[1:]]
        + [pltpu.SemaphoreType.DMA((len(arrays) + 2,))],
        compiler_params=pltpu.CompilerParams(vmem_limit_bytes=60 * 1024 * 1024),
    )(spots, *arrays)


def swap_rows(value):
    return lax.ppermute(value, "head", [(i, (i + 8) % 16) for i in range(16)])


def along_z(value, step):
    return lax.ppermute(
        value, "head", [(i, (i // 8) * 8 + (i + step) % 8) for i in range(16)]
    )


def along_seq(value, step):
    return lax.ppermute(value, "seq", [(i, i + step) for i in range(16 - step)])


def round_x(value, step):
    return lax.ppermute(value, "seq", [(i, (i + 4 * step) % 16) for i in range(16)])


def other_core(value):
    return lax.ppermute(value, "seq", [(i, i ^ 1) for i in range(16)])


def z_ring(value):
    found = [value]
    up = down = value
    for step in range(1, 5):
        up = along_z(up, 1)
        if step < 4:
            down = along_z(down, -1)
        if step < 4:
            up, down = lax.optimization_barrier((up, down))
            found += [up, down]
        else:
            found.append(up)
    return found


ROWS = [list(range(8)), list(range(8, 16))]


def sent_to_row(value):
    return lax.all_to_all(
        jnp.broadcast_to(value[None], (8, *value.shape)),
        "head", 0, 0, tiled=True, axis_index_groups=ROWS,
    )


def owned_piece(w_out, seq):
    x, core = seq >> 2, seq & 1
    rows, width = w_out.shape
    part = rows // 8
    piece = lax.dynamic_slice_in_dim(w_out, (2 * x + core) * part, part, 0)
    return piece.reshape(part, 2, 8, width // 16).transpose(2, 1, 0, 3)


def owned_columns(piece, seq, tie):
    x = seq >> 2
    moved = [round_x(piece, step) for step in (1, 3, 2)]
    *moved, tie = lax.optimization_barrier((*moved, tie))
    held = jnp.zeros((4, *piece.shape), piece.dtype)
    held = lax.dynamic_update_slice_in_dim(held, piece[None], x, 0)
    for step, part in zip((1, 3, 2), moved):
        held = lax.dynamic_update_slice_in_dim(held, part[None], (x - step) & 3, 0)
    return held, other_core(held), tie


def gather_rows(spot_ref, held, twin, spot, out, slot):
    core = spot_ref[1]
    part = held.shape[3]
    cols = held.shape[4]
    for x in range(4):
        for source, side in ((held, core), (twin, 1 - core)):
            low = pl.multiple_of(x * 2 * part + side * part, part)
            for half in range(2):
                out[slot, pl.ds(low, part), half * cols:(half + 1) * cols] = source[x, spot, half]


def finish_kernel(spot_ref, *refs):
    values, held, twin = refs[:7], refs[7], refs[8]
    part_out, tail_out, w_scr = refs[9:]
    total = None
    for k, value in enumerate(values):
        gather_rows(spot_ref, held, twin, (spot_ref[0] + OFFSETS[k]) & 7, w_scr, k)
        new = jnp.dot(value[...], w_scr[k], preferred_element_type=jnp.float32)
        total = new if total is None else total + new
    part_out[...] = total
    gather_rows(spot_ref, held, twin, (spot_ref[0] + OFFSETS[7]) & 7, tail_out, 0)


def close_kernel(spot_ref, part_ref, tail_ref, last_ref, mine_out, theirs_out):
    total = part_ref[...] + jnp.dot(last_ref[...], tail_ref[0], preferred_element_type=jnp.float32)
    cols = mine_out.shape[1]
    for row in range(2):

        @pl.when((spot_ref[0] >> 3) == row)
        def _():
            mine_out[...] = total[:, row * cols:(row + 1) * cols]
            theirs_out[...] = total[:, (1 - row) * cols:(2 - row) * cols].astype(jnp.bfloat16)


def finish(spots, values, held, twin):
    tok, feats = values[0].shape
    cols = held.shape[-1]
    limit = pltpu.CompilerParams(vmem_limit_bytes=24 * 1024 * 1024)
    smem = [pl.BlockSpec(memory_space=pltpu.SMEM)]
    part, tail = pl.pallas_call(
        finish_kernel,
        out_shape=(
            jax.ShapeDtypeStruct((tok, 2 * cols), jnp.float32),
            jax.ShapeDtypeStruct((1, feats, 2 * cols), held.dtype),
        ),
        in_specs=smem + in_vmem(9),
        out_specs=tuple(in_vmem(2)),
        scratch_shapes=[pltpu.VMEM((7, feats, 2 * cols), held.dtype)],
        compiler_params=limit,
    )(spots, *values[:7], held, twin)
    mine, theirs = pl.pallas_call(
        close_kernel,
        out_shape=(
            jax.ShapeDtypeStruct((tok, cols), jnp.float32),
            jax.ShapeDtypeStruct((tok, cols), jnp.bfloat16),
        ),
        in_specs=smem + in_vmem(3),
        out_specs=tuple(in_vmem(2)),
        compiler_params=limit,
    )(spots, part, tail, values[7])
    return (mine + swap_rows(theirs).astype(jnp.float32)).astype(jnp.bfloat16)


def body(tokens, w_query, w_keyval, w_out):
    tok_rows = tokens.shape[0]
    head = lax.axis_index("head").astype(jnp.int32)
    seq = lax.axis_index("seq").astype(jnp.int32)
    row, core = head >> 3, seq & 1
    spots = jnp.stack([head, core])
    half = w_query.shape[0] // 2
    quarter = half // 2
    kv_flat = w_keyval.T
    kv_part = swap_rows(lax.dynamic_slice_in_dim(kv_flat, (1 - row) * half, half, 1))
    q_same = swap_rows(
        lax.dynamic_slice_in_dim(w_query, (1 - row) * half + core * quarter, quarter, 0)
    )
    q_twin = other_core(q_same)
    kv_own = lax.dynamic_slice_in_dim(kv_flat, row * half, half, 1)
    shards = z_ring(tokens)
    piece, shards[5], shards[6] = lax.optimization_barrier(
        (owned_piece(w_out, seq), shards[5], shards[6])
    )
    piece = lax.all_to_all(piece, "head", 0, 0, tiled=True, axis_index_groups=ROWS)
    kv_part, q_mine, q_theirs = project(
        spots,
        (*shards, kv_own, kv_part, w_query, q_same, q_twin),
        ((2 * kv_flat.shape[0], tok_rows),) + ((tok_rows, w_query.shape[1]),) * 2,
    )
    kv = (kv_part + swap_rows(kv_part)).astype(jnp.bfloat16)
    piece, kv = lax.optimization_barrier((piece, kv))
    q_sent = swap_rows(q_theirs)
    near = along_seq(kv, 1)
    far = along_seq(kv[:kv_flat.shape[0]], 2)
    keyval = sent_to_row(jnp.concatenate([kv, near, far], axis=0))
    keyval = keyval.reshape(8, 5, kv_flat.shape[0], tok_rows)
    attended = attend(seq.reshape(1), q_mine, q_sent, keyval)
    values = z_ring(attended)
    held, twin, values[3] = owned_columns(piece, seq, values[3])
    return finish(spots, values, held, twin)


def solution(mesh):
    return jax.shard_map(
        body,
        mesh=mesh,
        in_specs=(P("seq", "head"), P(None, "head"), P(None, "head"), P("head", None)),
        out_specs=P("seq", "head"),
        check_vma=False,
    )
```

```python
import jax
import jax.numpy as jnp
from jax import lax
from jax.experimental import pallas as pl
from jax.experimental.pallas import tpu as pltpu
from jax.sharding import PartitionSpec as P


HEAD = 128
WIN1 = 512
WIN2 = 32
BLK = 128
GROUP = 16
MIX = 16
LOW = -1e30
LANES = (((1,), (1,)), ((), ()))


def pick(source, which, lanes):
    places = slice((which % 2) * 4, (which % 2) * 4 + 4)
    found = source[places, :, lanes] if len(source.shape) == 3 else source[places, which // 2, :, lanes]
    return found.reshape(HEAD, BLK)


def attend_kernel(
    seq_ref, mine_any, sent_any, far_ref, near_ref, own_ref, out_ref,
    k2f, v2f, ktile, vtile, kpair, vpair, s_scr, mx_scr, mcb_scr, mine_ref, sent_ref, sems,
):
    fetches = [
        pltpu.make_async_copy(source, target, sems.at[k])
        for k, (source, target) in enumerate(((mine_any, mine_ref), (sent_any, sent_ref)))
    ]
    for fetch in fetches:
        fetch.start()
    tok = mine_ref.shape[0]
    heads = mine_ref.shape[1] // HEAD
    blocks = tok // BLK
    seq = seq_ref[0]
    coef = (HEAD ** -0.5) * 1.4426950408889634
    start = seq == 0

    for t in range(6):
        source = (far_ref, near_ref, own_ref)[t // 2]
        lanes = slice((t % 2) * BLK, (t % 2 + 1) * BLK)
        ktile[t] = pick(source, 0, lanes)
        vtile[t] = pick(source, 1, lanes).astype(jnp.float32).T.astype(jnp.bfloat16)
    for scr, which in ((k2f, 2), (v2f, 3)):
        scr[:BLK] = pick(near_ref, which, slice(tok - BLK, tok)).astype(jnp.float32).T
        for t in range(blocks):
            scr[(t + 1) * BLK:(t + 2) * BLK] = pick(own_ref, which, slice(t * BLK, (t + 1) * BLK)).astype(jnp.float32).T

    @pl.when(start)
    def _():
        k2f[:BLK] = jnp.broadcast_to(k2f[BLK:BLK + 1], (BLK, HEAD))
        v2f[:BLK] = jnp.zeros((BLK, HEAD), jnp.float32)

    for fetch in fetches:
        fetch.wait()
    row = lax.broadcasted_iota(jnp.int32, (BLK, BLK), 0)
    col = lax.broadcasted_iota(jnp.int32, (BLK, BLK), 1)
    early = col > row
    absent = jnp.maximum(WIN1 - seq * tok, 0) // BLK

    def one(combo, _):
        h = combo // blocks
        b = combo % blocks
        base = pl.multiple_of(b * BLK, BLK)
        hcol = pl.multiple_of(h * HEAD, HEAD)
        at = (pl.ds(base, BLK), pl.ds(hcol, HEAD))
        qf = (mine_ref[at] + sent_ref[at]).astype(jnp.bfloat16).astype(jnp.float32)
        for slot, t in enumerate((0, 4, 1, 2, 3)):
            kpair[:, slot * BLK:(slot + 1) * BLK] = ktile[b + t]
            vpair[slot * BLK:(slot + 1) * BLK] = vtile[b + t]
        mx_scr[...] = jnp.full(mx_scr.shape, LOW, jnp.float32)

        def scores(step, _):
            lag0 = step * GROUP
            prods = []
            for g in range(GROUP):
                k2 = k2f[pl.ds(BLK + base - lag0 - g, BLK), :]
                prods.append((qf * k2).astype(jnp.bfloat16))
            prod = jnp.concatenate(prods, axis=0)
            for t in range(3):
                width = 2 * BLK if t < 2 else BLK
                s = jnp.dot(prod, kpair[:, 2 * BLK * t:2 * BLK * t + width], preferred_element_type=jnp.float32)
                s = s.reshape(GROUP, BLK, width)
                if t == 0:
                    parts = [(0, jnp.where(early[None], s[:, :, :BLK], s[:, :, BLK:]))]
                elif t == 1:
                    parts = [(1, s[:, :, :BLK]), (2, s[:, :, BLK:])]
                else:
                    parts = [(3, s)]
                for place, value in parts:
                    s_scr[pl.ds(lag0, GROUP), :, place * BLK:(place + 1) * BLK] = value
                    top = value[0]
                    for g in range(1, GROUP):
                        top = jnp.maximum(top, value[g])
                    mx_scr[place] = jnp.maximum(mx_scr[place], top)
            return 0

        lax.fori_loop(0, WIN2 // GROUP, scores, 0)
        tops = []
        gone = []
        for place in range(4):
            hide = (b + place) < absent
            mask = early if place == 0 else row >= 0
            gone.append(jnp.logical_and(mask, hide))
            tops.append(jnp.where(gone[place], LOW, mx_scr[place]))
        top = jnp.maximum(jnp.maximum(tops[0], tops[1]), jnp.maximum(tops[2], tops[3]))
        peak = jnp.max(top, axis=1, keepdims=True) * coef
        for place in range(4):
            mcb_scr[place] = jnp.where(gone[place], -LOW, jnp.broadcast_to(peak, (BLK, BLK)))

        def raised_at(lag):
            return [
                jnp.exp2(s_scr[lag, :, p * BLK:(p + 1) * BLK] * coef - mcb_scr[p])
                for p in range(4)
            ]

        def mix(step, carry):
            acc, tot = carry
            ws = []
            for g in range(MIX):
                raised = raised_at(step * MIX + g)
                tot = tot + ((raised[0] + raised[1]) + (raised[2] + raised[3]))
                split = [jnp.where(early, raised[0], 0.0), jnp.where(early, 0.0, raised[0])]
                ws.append(jnp.concatenate([part.astype(jnp.bfloat16) for part in split + raised[1:]], axis=1))
            m = jnp.dot(jnp.concatenate(ws, axis=0), vpair[...], preferred_element_type=jnp.float32)
            for g in range(MIX):
                acc = acc + m[g * BLK:(g + 1) * BLK] * v2f[pl.ds(BLK + base - step * MIX - g, BLK), :]
            return acc, tot

        zero = jnp.zeros((BLK, HEAD), jnp.float32)
        acc, tot = lax.fori_loop(0, WIN2 // MIX, mix, (zero, zero))
        last = raised_at(WIN2 - 1)
        spare = jnp.where(jnp.logical_and(start, b == 0), jnp.maximum(WIN2 - 1 - row, 0), 0)
        tot = tot - spare.astype(jnp.float32) * ((last[0] + last[1]) + (last[2] + last[3]))
        total = jnp.sum(tot, axis=1, keepdims=True)
        out_ref[at] = (acc / total).astype(jnp.bfloat16)
        return 0

    lax.fori_loop(0, heads * blocks, one, 0)


def in_vmem(count):
    return [pl.BlockSpec(memory_space=pltpu.VMEM)] * count


def attend(seq, mine, sent, far, near, own):
    tok = mine.shape[0]
    return pl.pallas_call(
        attend_kernel,
        out_shape=jax.ShapeDtypeStruct(mine.shape, jnp.bfloat16),
        in_specs=[pl.BlockSpec(memory_space=pltpu.SMEM)]
        + [pl.BlockSpec(memory_space=pltpu.HBM)] * 2
        + in_vmem(3),
        out_specs=in_vmem(1)[0],
        scratch_shapes=[
            pltpu.VMEM((BLK + tok, HEAD), jnp.float32),
            pltpu.VMEM((BLK + tok, HEAD), jnp.float32),
            pltpu.VMEM((6, HEAD, BLK), jnp.bfloat16),
            pltpu.VMEM((6, BLK, HEAD), jnp.bfloat16),
            pltpu.VMEM((HEAD, 5 * BLK), jnp.bfloat16),
            pltpu.VMEM((5 * BLK, HEAD), jnp.bfloat16),
            pltpu.VMEM((WIN2, BLK, 4 * BLK), jnp.float32),
            pltpu.VMEM((4, BLK, BLK), jnp.float32),
            pltpu.VMEM((4, BLK, BLK), jnp.float32),
            pltpu.VMEM(mine.shape, jnp.float32),
            pltpu.VMEM(mine.shape, jnp.float32),
            pltpu.SemaphoreType.DMA((2,)),
        ],
        compiler_params=pltpu.CompilerParams(vmem_limit_bytes=24 * 1024 * 1024),
    )(seq, mine, sent, far, near, own)


OFFSETS = (0, -1, 1, -2, 2, -3, 3, -4)


def project_kernel(spot_ref, *refs):
    shards_any, kv_any, own_any, parts_any = refs[:8], refs[8:10], refs[10], refs[11:13]
    kv_out, mine_any, theirs_any = refs[13:16]
    shards, kv_ref, own_ref, part_ref, mine_out, theirs_out, sems = refs[16:]
    depth = shards.shape[2]
    half = own_ref.shape[0]
    row, core = spot_ref[0] >> 3, spot_ref[1]
    parts = kv_ref.shape[0] // 2

    def rows_at(place, count):
        return pl.ds(pl.multiple_of(place * count, count), count)

    moves = [(source, shards.at[k]) for k, source in enumerate(shards_any)]
    for source, side in zip(kv_any, (row, 1 - row)):
        moves.append((source, kv_ref.at[rows_at(side, parts), :]))
    moves.append((own_any.at[rows_at(row, half), :], own_ref))
    for source, side in zip(parts_any, (core, 1 - core)):
        moves.append((source, part_ref.at[rows_at(side, half // 2), :]))
    fetches = [
        pltpu.make_async_copy(source, target, sems.at[k])
        for k, (source, target) in enumerate(moves)
    ]
    for fetch in fetches:
        fetch.start()
    spots = [(spot_ref[0] + offset) & 7 for offset in OFFSETS]
    for fetch in fetches[:10]:
        fetch.wait()
    total = None
    for k, spot in enumerate(spots):
        cols = kv_ref[:, rows_at(spot, depth)]
        new = lax.dot_general(cols, shards[k], LANES, preferred_element_type=jnp.float32)
        total = new if total is None else total + new
    kv_out[...] = total

    def whole_sum(weights, out, target, sem):
        total = None
        for k, spot in enumerate(spots):
            new = jnp.dot(shards[k], weights[rows_at(spot, depth), :], preferred_element_type=jnp.float32)
            total = new if total is None else total + new
        out[...] = total
        move = pltpu.make_async_copy(out, target, sem)
        move.start()
        return move

    fetches[10].wait()
    keep = whole_sum(own_ref, mine_out, mine_any, sems.at[13])
    for fetch in fetches[11:]:
        fetch.wait()
    send = whole_sum(part_ref, theirs_out, theirs_any, sems.at[14])
    keep.wait()
    send.wait()


def project(spots, arrays, shapes):
    far_off = pl.BlockSpec(memory_space=pltpu.HBM)
    own = arrays[10]
    half = (own.shape[0] // 2, own.shape[1])
    kept = [(8, *arrays[0].shape), (2 * arrays[8].shape[0], arrays[8].shape[1]), half, half]
    return pl.pallas_call(
        project_kernel,
        out_shape=tuple(jax.ShapeDtypeStruct(shape, jnp.float32) for shape in shapes),
        in_specs=[pl.BlockSpec(memory_space=pltpu.SMEM)] + [far_off] * len(arrays),
        out_specs=(in_vmem(1)[0], far_off, far_off),
        scratch_shapes=[pltpu.VMEM(shape, own.dtype) for shape in kept]
        + [pltpu.VMEM(shape, jnp.float32) for shape in shapes[1:]]
        + [pltpu.SemaphoreType.DMA((15,))],
        compiler_params=pltpu.CompilerParams(vmem_limit_bytes=60 * 1024 * 1024),
    )(spots, *arrays)


def swap_rows(value):
    return lax.ppermute(value, "head", [(i, (i + 8) % 16) for i in range(16)])


def along_z(value, step):
    return lax.ppermute(
        value, "head", [(i, (i // 8) * 8 + (i + step) % 8) for i in range(16)]
    )


def along_seq(value, step):
    return lax.ppermute(value, "seq", [(i, i + step) for i in range(16 - step)])


def round_x(value, step):
    return lax.ppermute(value, "seq", [(i, (i + 4 * step) % 16) for i in range(16)])


def other_core(value):
    return lax.ppermute(value, "seq", [(i, i ^ 1) for i in range(16)])


def z_ring(value, extra=None):
    found = [value]
    up = down = value
    for step in range(1, 5):
        up = along_z(up, 1)
        if step < 4:
            down = along_z(down, -1)
        if step < 4:
            if extra is not None and step == 2:
                up, down, extra = lax.optimization_barrier((up, down, extra))
            else:
                up, down = lax.optimization_barrier((up, down))
            found += [up, down]
        else:
            found.append(up)
    return found if extra is None else (found, extra)


ROWS = [list(range(8)), list(range(8, 16))]


def sent_to_row(value):
    return lax.all_to_all(
        jnp.broadcast_to(value[None], (8, *value.shape)),
        "head", 0, 0, tiled=True, axis_index_groups=ROWS,
    )


def owned_piece(w_out, seq):
    x, core = seq >> 2, seq & 1
    rows, width = w_out.shape
    part = rows // 8
    piece = lax.dynamic_slice_in_dim(w_out, (2 * x + core) * part, part, 0)
    return piece.reshape(part, 2, 8, width // 16).transpose(2, 1, 0, 3)


def owned_columns(piece, seq, tie):
    x = seq >> 2
    moved = [round_x(piece, step) for step in (1, 3, 2)]
    *moved, tie = lax.optimization_barrier((*moved, tie))
    held = jnp.zeros((4, *piece.shape), piece.dtype)
    held = lax.dynamic_update_slice_in_dim(held, piece[None], x, 0)
    for step, part in zip((1, 3, 2), moved):
        held = lax.dynamic_update_slice_in_dim(held, part[None], (x - step) & 3, 0)
    return held, other_core(held), tie


def gather_rows(spot_ref, held, twin, spot, out, slot):
    core = spot_ref[1]
    part = held.shape[3]
    cols = held.shape[4]
    for x in range(4):
        for source, side in ((held, core), (twin, 1 - core)):
            low = pl.multiple_of(x * 2 * part + side * part, part)
            for half in range(2):
                out[slot, pl.ds(low, part), half * cols:(half + 1) * cols] = source[x, spot, half]


def finish_kernel(spot_ref, *refs):
    values, held, twin = refs[:7], refs[7], refs[8]
    part_out, tail_out, w_scr = refs[9:]
    total = None
    for k, value in enumerate(values):
        gather_rows(spot_ref, held, twin, (spot_ref[0] + OFFSETS[k]) & 7, w_scr, k)
        new = jnp.dot(value[...], w_scr[k], preferred_element_type=jnp.float32)
        total = new if total is None else total + new
    part_out[...] = total
    gather_rows(spot_ref, held, twin, (spot_ref[0] + OFFSETS[7]) & 7, tail_out, 0)


def close_kernel(spot_ref, part_ref, tail_ref, last_ref, mine_out, theirs_out):
    total = part_ref[...] + jnp.dot(last_ref[...], tail_ref[0], preferred_element_type=jnp.float32)
    cols = mine_out.shape[1]
    for row in range(2):

        @pl.when((spot_ref[0] >> 3) == row)
        def _():
            mine_out[...] = total[:, row * cols:(row + 1) * cols]
            theirs_out[...] = total[:, (1 - row) * cols:(2 - row) * cols].astype(jnp.bfloat16)


def finish(spots, values, held, twin):
    tok, feats = values[0].shape
    cols = held.shape[-1]
    limit = pltpu.CompilerParams(vmem_limit_bytes=24 * 1024 * 1024)
    smem = [pl.BlockSpec(memory_space=pltpu.SMEM)]
    part, tail = pl.pallas_call(
        finish_kernel,
        out_shape=(
            jax.ShapeDtypeStruct((tok, 2 * cols), jnp.float32),
            jax.ShapeDtypeStruct((1, feats, 2 * cols), held.dtype),
        ),
        in_specs=smem + in_vmem(9),
        out_specs=tuple(in_vmem(2)),
        scratch_shapes=[pltpu.VMEM((7, feats, 2 * cols), held.dtype)],
        compiler_params=limit,
    )(spots, *values[:7], held, twin)
    mine, theirs = pl.pallas_call(
        close_kernel,
        out_shape=(
            jax.ShapeDtypeStruct((tok, cols), jnp.float32),
            jax.ShapeDtypeStruct((tok, cols), jnp.bfloat16),
        ),
        in_specs=smem + in_vmem(3),
        out_specs=tuple(in_vmem(2)),
        compiler_params=limit,
    )(spots, part, tail, values[7])
    return (mine + swap_rows(theirs).astype(jnp.float32)).astype(jnp.bfloat16)


def body(tokens, w_query, w_keyval, w_out):
    tok_rows = tokens.shape[0]
    head = lax.axis_index("head").astype(jnp.int32)
    seq = lax.axis_index("seq").astype(jnp.int32)
    row, core = head >> 3, seq & 1
    spots = jnp.stack([head, core])
    half = w_query.shape[0] // 2
    quarter = half // 2
    kv_flat = w_keyval.T
    kv_part = swap_rows(lax.dynamic_slice_in_dim(kv_flat, (1 - row) * half, half, 1))
    q_same = swap_rows(
        lax.dynamic_slice_in_dim(w_query, (1 - row) * half + core * quarter, quarter, 0)
    )
    q_twin = other_core(q_same)
    kv_own = lax.dynamic_slice_in_dim(kv_flat, row * half, half, 1)
    shards, piece = z_ring(tokens, owned_piece(w_out, seq))
    piece, shards[5], shards[6] = lax.optimization_barrier((piece, shards[5], shards[6]))
    piece = lax.all_to_all(piece, "head", 0, 0, tiled=True, axis_index_groups=ROWS)
    kv_part, q_mine, q_theirs = project(
        spots,
        (*shards, kv_own, kv_part, w_query, q_same, q_twin),
        ((2 * kv_flat.shape[0], tok_rows),) + ((tok_rows, w_query.shape[1]),) * 2,
    )
    kv = (kv_part + swap_rows(kv_part)).astype(jnp.bfloat16)
    piece, kv = lax.optimization_barrier((piece, kv))
    q_sent = swap_rows(q_theirs)
    keyval = sent_to_row(kv).reshape(8, 2, kv_flat.shape[0], tok_rows)
    near = along_seq(keyval, 1)
    far = along_seq(keyval[:, 0], 2)
    attended = attend(seq.reshape(1), q_mine, q_sent, far, near, keyval)
    values = z_ring(attended)
    held, twin, values[3] = owned_columns(piece, seq, values[3])
    return finish(spots, values, held, twin)


def solution(mesh):
    return jax.shard_map(
        body,
        mesh=mesh,
        in_specs=(P("seq", "head"), P(None, "head"), P(None, "head"), P("head", None)),
        out_specs=P("seq", "head"),
        check_vma=False,
    )
```

```python
import jax
import jax.numpy as jnp
from jax import lax
from jax.experimental import pallas as pl
from jax.experimental.pallas import tpu as pltpu
from jax.sharding import PartitionSpec as P


HEAD = 128
WIN1 = 512
WIN2 = 32
BLK = 128
GROUP = 32
MIX = 16
LOW = -1e30
LANES = (((1,), (1,)), ((), ()))


def pick(source, which, lanes):
    places = slice((which % 2) * 4, (which % 2) * 4 + 4)
    found = source[places, :, lanes] if len(source.shape) == 3 else source[places, which // 2, :, lanes]
    return found.reshape(HEAD, BLK)


def attend_kernel(
    seq_ref, mine_any, sent_any, far_ref, near_ref, own_ref, out_ref,
    k2f, v2f, ktile, vtile, kpair, vpair, s_scr, mx_scr, mcb_scr, mine_ref, sent_ref, sems,
):
    fetches = [
        pltpu.make_async_copy(source, target, sems.at[k])
        for k, (source, target) in enumerate(((mine_any, mine_ref), (sent_any, sent_ref)))
    ]
    for fetch in fetches:
        fetch.start()
    tok = mine_ref.shape[0]
    heads = mine_ref.shape[1] // HEAD
    blocks = tok // BLK
    seq = seq_ref[0]
    coef = (HEAD ** -0.5) * 1.4426950408889634
    start = seq == 0

    for t in range(6):
        source = (far_ref, near_ref, own_ref)[t // 2]
        lanes = slice((t % 2) * BLK, (t % 2 + 1) * BLK)
        ktile[t] = pick(source, 0, lanes)
        vtile[t] = pick(source, 1, lanes).astype(jnp.float32).T.astype(jnp.bfloat16)
    for scr, which in ((k2f, 2), (v2f, 3)):
        scr[:BLK] = pick(near_ref, which, slice(tok - BLK, tok)).astype(jnp.float32).T
        for t in range(blocks):
            scr[(t + 1) * BLK:(t + 2) * BLK] = pick(own_ref, which, slice(t * BLK, (t + 1) * BLK)).astype(jnp.float32).T

    @pl.when(start)
    def _():
        k2f[:BLK] = jnp.broadcast_to(k2f[BLK:BLK + 1], (BLK, HEAD))
        v2f[:BLK] = jnp.zeros((BLK, HEAD), jnp.float32)

    for fetch in fetches:
        fetch.wait()
    row = lax.broadcasted_iota(jnp.int32, (BLK, BLK), 0)
    col = lax.broadcasted_iota(jnp.int32, (BLK, BLK), 1)
    early = col > row
    absent = jnp.maximum(WIN1 - seq * tok, 0) // BLK

    def one(combo, _):
        h = combo // blocks
        b = combo % blocks
        base = pl.multiple_of(b * BLK, BLK)
        hcol = pl.multiple_of(h * HEAD, HEAD)
        at = (pl.ds(base, BLK), pl.ds(hcol, HEAD))
        qf = (mine_ref[at] + sent_ref[at]).astype(jnp.bfloat16).astype(jnp.float32)
        for slot, t in enumerate((0, 4, 1, 2, 3)):
            kpair[:, slot * BLK:(slot + 1) * BLK] = ktile[b + t]
            vpair[slot * BLK:(slot + 1) * BLK] = vtile[b + t]
        mx_scr[...] = jnp.full(mx_scr.shape, LOW, jnp.float32)

        def scores(step, _):
            lag0 = step * GROUP
            prods = []
            for g in range(GROUP):
                k2 = k2f[pl.ds(BLK + base - lag0 - g, BLK), :]
                prods.append((qf * k2).astype(jnp.bfloat16))
            prod = jnp.concatenate(prods, axis=0)
            for t in range(3):
                width = 2 * BLK if t < 2 else BLK
                s = jnp.dot(prod, kpair[:, 2 * BLK * t:2 * BLK * t + width], preferred_element_type=jnp.float32)
                s = s.reshape(GROUP, BLK, width)
                if t == 0:
                    parts = [(0, jnp.where(early[None], s[:, :, :BLK], s[:, :, BLK:]))]
                elif t == 1:
                    parts = [(1, s[:, :, :BLK]), (2, s[:, :, BLK:])]
                else:
                    parts = [(3, s)]
                for place, value in parts:
                    s_scr[pl.ds(lag0, GROUP), :, place * BLK:(place + 1) * BLK] = value
                    top = value[0]
                    for g in range(1, GROUP):
                        top = jnp.maximum(top, value[g])
                    mx_scr[place] = jnp.maximum(mx_scr[place], top)
            return 0

        lax.fori_loop(0, WIN2 // GROUP, scores, 0)
        tops = []
        gone = []
        for place in range(4):
            hide = (b + place) < absent
            mask = early if place == 0 else row >= 0
            gone.append(jnp.logical_and(mask, hide))
            tops.append(jnp.where(gone[place], LOW, mx_scr[place]))
        top = jnp.maximum(jnp.maximum(tops[0], tops[1]), jnp.maximum(tops[2], tops[3]))
        peak = jnp.max(top, axis=1, keepdims=True) * coef
        for place in range(4):
            mcb_scr[place] = jnp.where(gone[place], -LOW, jnp.broadcast_to(peak, (BLK, BLK)))

        def raised_at(lag):
            return [
                jnp.exp2(s_scr[lag, :, p * BLK:(p + 1) * BLK] * coef - mcb_scr[p])
                for p in range(4)
            ]

        def mix(step, carry):
            acc, tot = carry
            ws = []
            for g in range(MIX):
                raised = raised_at(step * MIX + g)
                tot = tot + ((raised[0] + raised[1]) + (raised[2] + raised[3]))
                split = [jnp.where(early, raised[0], 0.0), jnp.where(early, 0.0, raised[0])]
                ws.append(jnp.concatenate([part.astype(jnp.bfloat16) for part in split + raised[1:]], axis=1))
            m = jnp.dot(jnp.concatenate(ws, axis=0), vpair[...], preferred_element_type=jnp.float32)
            for g in range(MIX):
                acc = acc + m[g * BLK:(g + 1) * BLK] * v2f[pl.ds(BLK + base - step * MIX - g, BLK), :]
            return acc, tot

        zero = jnp.zeros((BLK, HEAD), jnp.float32)
        acc, tot = lax.fori_loop(0, WIN2 // MIX, mix, (zero, zero))
        last = raised_at(WIN2 - 1)
        spare = jnp.where(jnp.logical_and(start, b == 0), jnp.maximum(WIN2 - 1 - row, 0), 0)
        tot = tot - spare.astype(jnp.float32) * ((last[0] + last[1]) + (last[2] + last[3]))
        total = jnp.sum(tot, axis=1, keepdims=True)
        out_ref[at] = (acc / total).astype(jnp.bfloat16)
        return 0

    lax.fori_loop(0, heads * blocks, one, 0)


def in_vmem(count):
    return [pl.BlockSpec(memory_space=pltpu.VMEM)] * count


def attend(seq, mine, sent, far, near, own):
    tok = mine.shape[0]
    return pl.pallas_call(
        attend_kernel,
        out_shape=jax.ShapeDtypeStruct(mine.shape, jnp.bfloat16),
        in_specs=[pl.BlockSpec(memory_space=pltpu.SMEM)]
        + [pl.BlockSpec(memory_space=pltpu.HBM)] * 2
        + in_vmem(3),
        out_specs=in_vmem(1)[0],
        scratch_shapes=[
            pltpu.VMEM((BLK + tok, HEAD), jnp.float32),
            pltpu.VMEM((BLK + tok, HEAD), jnp.float32),
            pltpu.VMEM((6, HEAD, BLK), jnp.bfloat16),
            pltpu.VMEM((6, BLK, HEAD), jnp.bfloat16),
            pltpu.VMEM((HEAD, 5 * BLK), jnp.bfloat16),
            pltpu.VMEM((5 * BLK, HEAD), jnp.bfloat16),
            pltpu.VMEM((WIN2, BLK, 4 * BLK), jnp.float32),
            pltpu.VMEM((4, BLK, BLK), jnp.float32),
            pltpu.VMEM((4, BLK, BLK), jnp.float32),
            pltpu.VMEM(mine.shape, jnp.float32),
            pltpu.VMEM(mine.shape, jnp.float32),
            pltpu.SemaphoreType.DMA((2,)),
        ],
        compiler_params=pltpu.CompilerParams(vmem_limit_bytes=24 * 1024 * 1024),
    )(seq, mine, sent, far, near, own)


OFFSETS = (0, -1, 1, -2, 2, -3, 3, -4)


def project_kernel(spot_ref, *refs):
    shards_any, kv_any, own_any, parts_any = refs[:8], refs[8:10], refs[10], refs[11:13]
    kv_out, mine_any, theirs_any = refs[13:16]
    rows_ref, kv_ref, own_ref, part_ref, mine_out, theirs_out, sems = refs[16:]
    depth = shards_any[0].shape[1]
    half = own_ref.shape[0]
    row, core = spot_ref[0] >> 3, spot_ref[1]
    parts = kv_ref.shape[0] // 2

    def at(place, count):
        return pl.ds(pl.multiple_of(place * count, count), count)

    moves = []
    for offset, source in zip(OFFSETS, shards_any):
        moves.append((source, rows_ref.at[:, at((spot_ref[0] + offset) & 7, depth)]))
    for source, side in zip(kv_any, (row, 1 - row)):
        moves.append((source, kv_ref.at[at(side, parts), :]))
    moves.append((own_any.at[at(row, half), :], own_ref))
    for source, side in zip(parts_any, (core, 1 - core)):
        moves.append((source, part_ref.at[at(side, half // 2), :]))
    fetches = [
        pltpu.make_async_copy(source, target, sems.at[k])
        for k, (source, target) in enumerate(moves)
    ]
    for fetch in fetches:
        fetch.start()
    for fetch in fetches[:10]:
        fetch.wait()
    kv_out[...] = lax.dot_general(kv_ref[...], rows_ref[...], LANES, preferred_element_type=jnp.float32)
    fetches[10].wait()
    mine_out[...] = jnp.dot(rows_ref[...], own_ref[...], preferred_element_type=jnp.float32)
    keep = pltpu.make_async_copy(mine_out, mine_any, sems.at[13])
    keep.start()
    for fetch in fetches[11:]:
        fetch.wait()
    theirs_out[...] = jnp.dot(rows_ref[...], part_ref[...], preferred_element_type=jnp.float32)
    send = pltpu.make_async_copy(theirs_out, theirs_any, sems.at[14])
    send.start()
    keep.wait()
    send.wait()


def project(spots, arrays, shapes):
    far_off = pl.BlockSpec(memory_space=pltpu.HBM)
    own = arrays[10]
    half = (own.shape[0] // 2, own.shape[1])
    kept = [(arrays[0].shape[0], half[0]), (2 * arrays[8].shape[0], arrays[8].shape[1]), half, half]
    return pl.pallas_call(
        project_kernel,
        out_shape=tuple(jax.ShapeDtypeStruct(shape, jnp.float32) for shape in shapes),
        in_specs=[pl.BlockSpec(memory_space=pltpu.SMEM)] + [far_off] * len(arrays),
        out_specs=(in_vmem(1)[0], far_off, far_off),
        scratch_shapes=[pltpu.VMEM(shape, own.dtype) for shape in kept]
        + [pltpu.VMEM(shape, jnp.float32) for shape in shapes[1:]]
        + [pltpu.SemaphoreType.DMA((15,))],
        compiler_params=pltpu.CompilerParams(vmem_limit_bytes=60 * 1024 * 1024),
    )(spots, *arrays)


def swap_rows(value):
    return lax.ppermute(value, "head", [(i, (i + 8) % 16) for i in range(16)])


def along_z(value, step):
    return lax.ppermute(
        value, "head", [(i, (i // 8) * 8 + (i + step) % 8) for i in range(16)]
    )


def along_seq(value, step):
    return lax.ppermute(value, "seq", [(i, i + step) for i in range(16 - step)])


def round_x(value, step):
    return lax.ppermute(value, "seq", [(i, (i + 4 * step) % 16) for i in range(16)])


def other_core(value):
    return lax.ppermute(value, "seq", [(i, i ^ 1) for i in range(16)])


def z_ring(value, extra=None):
    found = [value]
    up = down = value
    for step in range(1, 5):
        up = along_z(up, 1)
        if step < 4:
            down = along_z(down, -1)
        if step < 4:
            if extra is not None and step == 2:
                up, down, *extra = lax.optimization_barrier((up, down, *extra))
            else:
                up, down = lax.optimization_barrier((up, down))
            found += [up, down]
        else:
            found.append(up)
    return found if extra is None else (found, extra)


ROWS = [list(range(8)), list(range(8, 16))]


def sent_to_row(value):
    return lax.all_to_all(
        jnp.broadcast_to(value[None], (8, *value.shape)),
        "head", 0, 0, tiled=True, axis_index_groups=ROWS,
    )


def owned_piece(w_out, seq):
    x, core = seq >> 2, seq & 1
    rows, width = w_out.shape
    part = rows // 8
    piece = lax.dynamic_slice_in_dim(w_out, (2 * x + core) * part, part, 0)
    return piece.reshape(part, 2, 8, width // 16).transpose(2, 1, 0, 3)


def owned_columns(piece, seq, tie):
    x = seq >> 2
    moved = [round_x(piece, step) for step in (1, 3, 2)]
    *moved, tie = lax.optimization_barrier((*moved, tie))
    held = jnp.zeros((4, *piece.shape), piece.dtype)
    held = lax.dynamic_update_slice_in_dim(held, piece[None], x, 0)
    for step, part in zip((1, 3, 2), moved):
        held = lax.dynamic_update_slice_in_dim(held, part[None], (x - step) & 3, 0)
    return held, other_core(held), tie


def gather_rows(spot_ref, held, twin, spot, out, slot):
    core = spot_ref[1]
    part = held.shape[3]
    cols = held.shape[4]
    for x in range(4):
        for source, side in ((held, core), (twin, 1 - core)):
            low = pl.multiple_of(x * 2 * part + side * part, part)
            for half in range(2):
                out[slot, pl.ds(low, part), half * cols:(half + 1) * cols] = source[x, spot, half]


def finish_kernel(spot_ref, *refs):
    values, held, twin = refs[:7], refs[7], refs[8]
    part_out, tail_out, w_scr = refs[9:]
    total = None
    for k, value in enumerate(values):
        gather_rows(spot_ref, held, twin, (spot_ref[0] + OFFSETS[k]) & 7, w_scr, k)
        new = jnp.dot(value[...], w_scr[k], preferred_element_type=jnp.float32)
        total = new if total is None else total + new
    part_out[...] = total
    gather_rows(spot_ref, held, twin, (spot_ref[0] + OFFSETS[7]) & 7, tail_out, 0)


def close_kernel(spot_ref, part_ref, tail_ref, last_ref, mine_out, theirs_out):
    total = part_ref[...] + jnp.dot(last_ref[...], tail_ref[0], preferred_element_type=jnp.float32)
    cols = mine_out.shape[1]
    for row in range(2):

        @pl.when((spot_ref[0] >> 3) == row)
        def _():
            mine_out[...] = total[:, row * cols:(row + 1) * cols]
            theirs_out[...] = total[:, (1 - row) * cols:(2 - row) * cols].astype(jnp.bfloat16)


def finish(spots, values, held, twin):
    tok, feats = values[0].shape
    cols = held.shape[-1]
    limit = pltpu.CompilerParams(vmem_limit_bytes=24 * 1024 * 1024)
    smem = [pl.BlockSpec(memory_space=pltpu.SMEM)]
    part, tail = pl.pallas_call(
        finish_kernel,
        out_shape=(
            jax.ShapeDtypeStruct((tok, 2 * cols), jnp.float32),
            jax.ShapeDtypeStruct((1, feats, 2 * cols), held.dtype),
        ),
        in_specs=smem + in_vmem(9),
        out_specs=tuple(in_vmem(2)),
        scratch_shapes=[pltpu.VMEM((7, feats, 2 * cols), held.dtype)],
        compiler_params=limit,
    )(spots, *values[:7], held, twin)
    mine, theirs = pl.pallas_call(
        close_kernel,
        out_shape=(
            jax.ShapeDtypeStruct((tok, cols), jnp.float32),
            jax.ShapeDtypeStruct((tok, cols), jnp.bfloat16),
        ),
        in_specs=smem + in_vmem(3),
        out_specs=tuple(in_vmem(2)),
        compiler_params=limit,
    )(spots, part, tail, values[7])
    return (mine + swap_rows(theirs).astype(jnp.float32)).astype(jnp.bfloat16)


def body(tokens, w_query, w_keyval, w_out):
    tok_rows = tokens.shape[0]
    head = lax.axis_index("head").astype(jnp.int32)
    seq = lax.axis_index("seq").astype(jnp.int32)
    row, core = head >> 3, seq & 1
    spots = jnp.stack([head, core])
    half = w_query.shape[0] // 2
    quarter = half // 2
    kv_flat = w_keyval.T
    kv_part = swap_rows(lax.dynamic_slice_in_dim(kv_flat, (1 - row) * half, half, 1))
    q_same = swap_rows(
        lax.dynamic_slice_in_dim(w_query, (1 - row) * half + core * quarter, quarter, 0)
    )
    q_twin = other_core(q_same)
    kv_own = lax.dynamic_slice_in_dim(kv_flat, row * half, half, 1)
    shards, (piece, spots) = z_ring(tokens, (owned_piece(w_out, seq), spots))
    piece = lax.all_to_all(piece, "head", 0, 0, tiled=True, axis_index_groups=ROWS)
    kv_part, q_mine, q_theirs = project(
        spots,
        (*shards, kv_own, kv_part, w_query, q_same, q_twin),
        ((2 * kv_flat.shape[0], tok_rows),) + ((tok_rows, w_query.shape[1]),) * 2,
    )
    kv_sent = swap_rows(kv_part)
    piece, kv_sent = lax.optimization_barrier((piece, kv_sent))
    kv = (kv_part + kv_sent).astype(jnp.bfloat16)
    q_sent = swap_rows(q_theirs)
    keyval = sent_to_row(kv).reshape(8, 2, kv_flat.shape[0], tok_rows)
    near = along_seq(keyval, 1)
    far = along_seq(keyval[:, 0], 2)
    attended = attend(seq.reshape(1), q_mine, q_sent, far, near, keyval)
    values = z_ring(attended)
    held, twin, values[3] = owned_columns(piece, seq, values[3])
    return finish(spots, values, held, twin)


def solution(mesh):
    return jax.shard_map(
        body,
        mesh=mesh,
        in_specs=(P("seq", "head"), P(None, "head"), P(None, "head"), P("head", None)),
        out_specs=P("seq", "head"),
        check_vma=False,
    )
```

```python
import jax
import jax.numpy as jnp
from jax import lax
from jax.experimental import pallas as pl
from jax.experimental.pallas import tpu as pltpu
from jax.sharding import PartitionSpec as P


HEAD = 128
WIN1 = 512
WIN2 = 32
BLK = 128
GROUP = 32
MIX = 16
LOW = -1e30
LANES = (((1,), (1,)), ((), ()))


def pick(source, which, lanes):
    places = slice((which % 2) * 4, (which % 2) * 4 + 4)
    found = source[places, :, lanes] if len(source.shape) == 3 else source[places, which // 2, :, lanes]
    return found.reshape(HEAD, BLK)


def attend_kernel(
    seq_ref, mine_any, sent_any, far_ref, near_ref, own_ref, out_ref,
    k2f, v2f, ktile, vtile, kpair, vpair, s_scr, mx_scr, mcb_scr, mine_ref, sent_ref, sems,
):
    fetches = [
        pltpu.make_async_copy(source, target, sems.at[k])
        for k, (source, target) in enumerate(((mine_any, mine_ref), (sent_any, sent_ref)))
    ]
    for fetch in fetches:
        fetch.start()
    tok = mine_ref.shape[0]
    heads = mine_ref.shape[1] // HEAD
    blocks = tok // BLK
    seq = seq_ref[0]
    coef = (HEAD ** -0.5) * 1.4426950408889634
    start = seq == 0

    for t in range(6):
        source = (far_ref, near_ref, own_ref)[t // 2]
        lanes = slice((t % 2) * BLK, (t % 2 + 1) * BLK)
        ktile[t] = pick(source, 0, lanes)
        vtile[t] = pick(source, 1, lanes).astype(jnp.float32).T.astype(jnp.bfloat16)
    for scr, which in ((k2f, 2), (v2f, 3)):
        scr[:BLK] = pick(near_ref, which, slice(tok - BLK, tok)).astype(jnp.float32).T
        for t in range(blocks):
            scr[(t + 1) * BLK:(t + 2) * BLK] = pick(own_ref, which, slice(t * BLK, (t + 1) * BLK)).astype(jnp.float32).T

    @pl.when(start)
    def _():
        k2f[:BLK] = jnp.broadcast_to(k2f[BLK:BLK + 1], (BLK, HEAD))
        v2f[:BLK] = jnp.zeros((BLK, HEAD), jnp.float32)

    for fetch in fetches:
        fetch.wait()
    row = lax.broadcasted_iota(jnp.int32, (BLK, BLK), 0)
    col = lax.broadcasted_iota(jnp.int32, (BLK, BLK), 1)
    early = col > row
    absent = jnp.maximum(WIN1 - seq * tok, 0) // BLK

    def one(combo, _):
        h = combo // blocks
        b = combo % blocks
        base = pl.multiple_of(b * BLK, BLK)
        hcol = pl.multiple_of(h * HEAD, HEAD)
        at = (pl.ds(base, BLK), pl.ds(hcol, HEAD))
        qf = (mine_ref[at] + sent_ref[at]).astype(jnp.bfloat16).astype(jnp.float32)
        for slot, t in enumerate((0, 4, 1, 2, 3)):
            kpair[:, slot * BLK:(slot + 1) * BLK] = ktile[b + t]
            vpair[slot * BLK:(slot + 1) * BLK] = vtile[b + t]
        mx_scr[...] = jnp.full(mx_scr.shape, LOW, jnp.float32)

        def scores(step, _):
            lag0 = step * GROUP
            prods = []
            for g in range(GROUP):
                k2 = k2f[pl.ds(BLK + base - lag0 - g, BLK), :]
                prods.append((qf * k2).astype(jnp.bfloat16))
            prod = jnp.concatenate(prods, axis=0)
            for t in range(3):
                width = 2 * BLK if t < 2 else BLK
                s = jnp.dot(prod, kpair[:, 2 * BLK * t:2 * BLK * t + width], preferred_element_type=jnp.float32)
                s = s.reshape(GROUP, BLK, width)
                if t == 0:
                    parts = [(0, jnp.where(early[None], s[:, :, :BLK], s[:, :, BLK:]))]
                elif t == 1:
                    parts = [(1, s[:, :, :BLK]), (2, s[:, :, BLK:])]
                else:
                    parts = [(3, s)]
                for place, value in parts:
                    s_scr[pl.ds(lag0, GROUP), :, place * BLK:(place + 1) * BLK] = value
                    top = value[0]
                    for g in range(1, GROUP):
                        top = jnp.maximum(top, value[g])
                    mx_scr[place] = jnp.maximum(mx_scr[place], top)
            return 0

        lax.fori_loop(0, WIN2 // GROUP, scores, 0)
        tops = []
        gone = []
        for place in range(4):
            hide = (b + place) < absent
            mask = early if place == 0 else row >= 0
            gone.append(jnp.logical_and(mask, hide))
            tops.append(jnp.where(gone[place], LOW, mx_scr[place]))
        top = jnp.maximum(jnp.maximum(tops[0], tops[1]), jnp.maximum(tops[2], tops[3]))
        peak = jnp.max(top, axis=1, keepdims=True) * coef
        for place in range(4):
            mcb_scr[place] = jnp.where(gone[place], -LOW, jnp.broadcast_to(peak, (BLK, BLK)))

        def raised_at(lag):
            return [
                jnp.exp2(s_scr[lag, :, p * BLK:(p + 1) * BLK] * coef - mcb_scr[p])
                for p in range(4)
            ]

        def mix(step, carry):
            acc, tot = carry
            ws = []
            for g in range(MIX):
                raised = raised_at(step * MIX + g)
                tot = tot + ((raised[0] + raised[1]) + (raised[2] + raised[3]))
                split = [jnp.where(early, raised[0], 0.0), jnp.where(early, 0.0, raised[0])]
                ws.append(jnp.concatenate([part.astype(jnp.bfloat16) for part in split + raised[1:]], axis=1))
            m = jnp.dot(jnp.concatenate(ws, axis=0), vpair[...], preferred_element_type=jnp.float32)
            for g in range(MIX):
                acc = acc + m[g * BLK:(g + 1) * BLK] * v2f[pl.ds(BLK + base - step * MIX - g, BLK), :]
            return acc, tot

        zero = jnp.zeros((BLK, HEAD), jnp.float32)
        acc, tot = lax.fori_loop(0, WIN2 // MIX, mix, (zero, zero))
        last = raised_at(WIN2 - 1)
        spare = jnp.where(jnp.logical_and(start, b == 0), jnp.maximum(WIN2 - 1 - row, 0), 0)
        tot = tot - spare.astype(jnp.float32) * ((last[0] + last[1]) + (last[2] + last[3]))
        total = jnp.sum(tot, axis=1, keepdims=True)
        out_ref[at] = (acc / total).astype(jnp.bfloat16)
        return 0

    lax.fori_loop(0, heads * blocks, one, 0)


def in_vmem(count):
    return [pl.BlockSpec(memory_space=pltpu.VMEM)] * count


def attend(seq, mine, sent, far, near, own):
    tok = mine.shape[0]
    return pl.pallas_call(
        attend_kernel,
        out_shape=jax.ShapeDtypeStruct(mine.shape, jnp.bfloat16),
        in_specs=[pl.BlockSpec(memory_space=pltpu.SMEM)]
        + [pl.BlockSpec(memory_space=pltpu.HBM)] * 2
        + in_vmem(3),
        out_specs=in_vmem(1)[0],
        scratch_shapes=[
            pltpu.VMEM((BLK + tok, HEAD), jnp.float32),
            pltpu.VMEM((BLK + tok, HEAD), jnp.float32),
            pltpu.VMEM((6, HEAD, BLK), jnp.bfloat16),
            pltpu.VMEM((6, BLK, HEAD), jnp.bfloat16),
            pltpu.VMEM((HEAD, 5 * BLK), jnp.bfloat16),
            pltpu.VMEM((5 * BLK, HEAD), jnp.bfloat16),
            pltpu.VMEM((WIN2, BLK, 4 * BLK), jnp.float32),
            pltpu.VMEM((4, BLK, BLK), jnp.float32),
            pltpu.VMEM((4, BLK, BLK), jnp.float32),
            pltpu.VMEM(mine.shape, jnp.float32),
            pltpu.VMEM(mine.shape, jnp.float32),
            pltpu.SemaphoreType.DMA((2,)),
        ],
        compiler_params=pltpu.CompilerParams(vmem_limit_bytes=24 * 1024 * 1024),
    )(seq, mine, sent, far, near, own)


OFFSETS = (0, -1, 1, -2, 2, -3, 3, -4)


def project_kernel(spot_ref, *refs):
    shards_any, kv_any, own_any, parts_any = refs[:8], refs[8:10], refs[10], refs[11:13]
    kv_out, mine_any, theirs_any = refs[13:16]
    rows_ref, kv_ref, own_ref, part_ref, mine_out, theirs_out, sems = refs[16:]
    depth = shards_any[0].shape[1]
    half = own_ref.shape[0]
    row, core = spot_ref[0] >> 3, spot_ref[1]
    parts = kv_ref.shape[0] // 2

    def at(place, count):
        return pl.ds(pl.multiple_of(place * count, count), count)

    moves = []
    for offset, source in zip(OFFSETS, shards_any):
        moves.append((source, rows_ref.at[:, at((spot_ref[0] + offset) & 7, depth)]))
    for source, side in zip(kv_any, (row, 1 - row)):
        moves.append((source, kv_ref.at[at(side, parts), :]))
    moves.append((own_any.at[at(row, half), :], own_ref))
    for source, side in zip(parts_any, (core, 1 - core)):
        moves.append((source, part_ref.at[at(side, half // 2), :]))
    fetches = [
        pltpu.make_async_copy(source, target, sems.at[k])
        for k, (source, target) in enumerate(moves)
    ]
    for fetch in fetches:
        fetch.start()
    for fetch in fetches[:10]:
        fetch.wait()
    kv_out[...] = lax.dot_general(
        rows_ref[...], kv_ref[...], LANES, preferred_element_type=jnp.float32
    ).T
    fetches[10].wait()
    mine_out[...] = jnp.dot(rows_ref[...], own_ref[...], preferred_element_type=jnp.float32)
    keep = pltpu.make_async_copy(mine_out, mine_any, sems.at[13])
    keep.start()
    for fetch in fetches[11:]:
        fetch.wait()
    theirs_out[...] = jnp.dot(rows_ref[...], part_ref[...], preferred_element_type=jnp.float32)
    send = pltpu.make_async_copy(theirs_out, theirs_any, sems.at[14])
    send.start()
    keep.wait()
    send.wait()


def project(spots, arrays, shapes):
    far_off = pl.BlockSpec(memory_space=pltpu.HBM)
    own = arrays[10]
    half = (own.shape[0] // 2, own.shape[1])
    kept = [(arrays[0].shape[0], half[0]), (2 * arrays[8].shape[0], arrays[8].shape[1]), half, half]
    return pl.pallas_call(
        project_kernel,
        out_shape=tuple(jax.ShapeDtypeStruct(shape, jnp.float32) for shape in shapes),
        in_specs=[pl.BlockSpec(memory_space=pltpu.SMEM)] + [far_off] * len(arrays),
        out_specs=(in_vmem(1)[0], far_off, far_off),
        scratch_shapes=[pltpu.VMEM(shape, own.dtype) for shape in kept]
        + [pltpu.VMEM(shape, jnp.float32) for shape in shapes[1:]]
        + [pltpu.SemaphoreType.DMA((15,))],
        compiler_params=pltpu.CompilerParams(vmem_limit_bytes=60 * 1024 * 1024),
    )(spots, *arrays)


def swap_rows(value):
    return lax.ppermute(value, "head", [(i, (i + 8) % 16) for i in range(16)])


def along_z(value, step):
    return lax.ppermute(
        value, "head", [(i, (i // 8) * 8 + (i + step) % 8) for i in range(16)]
    )


def along_seq(value, step):
    return lax.ppermute(value, "seq", [(i, i + step) for i in range(16 - step)])


def round_x(value, step):
    return lax.ppermute(value, "seq", [(i, (i + 4 * step) % 16) for i in range(16)])


def other_core(value):
    return lax.ppermute(value, "seq", [(i, i ^ 1) for i in range(16)])


def z_ring(value, extra=None):
    found = [value]
    up = down = value
    for step in range(1, 5):
        up = along_z(up, 1)
        if step < 4:
            down = along_z(down, -1)
        if step < 4:
            if extra is not None and step == 2:
                up, down, *extra = lax.optimization_barrier((up, down, *extra))
            else:
                up, down = lax.optimization_barrier((up, down))
            found += [up, down]
        else:
            found.append(up)
    return found if extra is None else (found, extra)


ROWS = [list(range(8)), list(range(8, 16))]


def copies_kernel(one_ref, two_ref, out_ref):
    total = (one_ref[...] + two_ref[...]).astype(out_ref.dtype)
    for k in range(out_ref.shape[0]):
        out_ref[k] = total


def sent_to_row(one, two):
    copies = pl.pallas_call(
        copies_kernel,
        out_shape=jax.ShapeDtypeStruct((8, *one.shape), jnp.bfloat16),
        in_specs=in_vmem(2),
        out_specs=in_vmem(1)[0],
        compiler_params=pltpu.CompilerParams(vmem_limit_bytes=8 * 1024 * 1024),
    )(one, two)
    return lax.all_to_all(copies, "head", 0, 0, tiled=True, axis_index_groups=ROWS)


def owned_piece(w_out, seq):
    x, core = seq >> 2, seq & 1
    rows, width = w_out.shape
    part = rows // 8
    piece = lax.dynamic_slice_in_dim(w_out, (2 * x + core) * part, part, 0)
    return piece.reshape(part, 2, 8, width // 16).transpose(2, 1, 0, 3)


def owned_columns(piece, seq, tie):
    x = seq >> 2
    moved = [round_x(piece, step) for step in (1, 3, 2)]
    *moved, tie = lax.optimization_barrier((*moved, tie))
    held = jnp.zeros((4, *piece.shape), piece.dtype)
    held = lax.dynamic_update_slice_in_dim(held, piece[None], x, 0)
    for step, part in zip((1, 3, 2), moved):
        held = lax.dynamic_update_slice_in_dim(held, part[None], (x - step) & 3, 0)
    return held, other_core(held), tie


def gather_rows(spot_ref, held, twin, spot, out, slot):
    core = spot_ref[1]
    part = held.shape[3]
    cols = held.shape[4]
    for x in range(4):
        for source, side in ((held, core), (twin, 1 - core)):
            low = pl.multiple_of(x * 2 * part + side * part, part)
            for half in range(2):
                out[slot, pl.ds(low, part), half * cols:(half + 1) * cols] = source[x, spot, half]


def finish_kernel(spot_ref, *refs):
    values, held, twin = refs[:7], refs[7], refs[8]
    part_out, tail_out, w_scr = refs[9:]
    total = None
    for k, value in enumerate(values):
        gather_rows(spot_ref, held, twin, (spot_ref[0] + OFFSETS[k]) & 7, w_scr, k)
        new = jnp.dot(value[...], w_scr[k], preferred_element_type=jnp.float32)
        total = new if total is None else total + new
    part_out[...] = total
    gather_rows(spot_ref, held, twin, (spot_ref[0] + OFFSETS[7]) & 7, tail_out, 0)


def close_kernel(spot_ref, part_ref, tail_ref, last_ref, mine_out, theirs_out):
    total = part_ref[...] + jnp.dot(last_ref[...], tail_ref[0], preferred_element_type=jnp.float32)
    cols = mine_out.shape[1]
    for row in range(2):

        @pl.when((spot_ref[0] >> 3) == row)
        def _():
            mine_out[...] = total[:, row * cols:(row + 1) * cols]
            theirs_out[...] = total[:, (1 - row) * cols:(2 - row) * cols].astype(jnp.bfloat16)


def finish(spots, values, held, twin):
    tok, feats = values[0].shape
    cols = held.shape[-1]
    limit = pltpu.CompilerParams(vmem_limit_bytes=24 * 1024 * 1024)
    smem = [pl.BlockSpec(memory_space=pltpu.SMEM)]
    part, tail = pl.pallas_call(
        finish_kernel,
        out_shape=(
            jax.ShapeDtypeStruct((tok, 2 * cols), jnp.float32),
            jax.ShapeDtypeStruct((1, feats, 2 * cols), held.dtype),
        ),
        in_specs=smem + in_vmem(9),
        out_specs=tuple(in_vmem(2)),
        scratch_shapes=[pltpu.VMEM((7, feats, 2 * cols), held.dtype)],
        compiler_params=limit,
    )(spots, *values[:7], held, twin)
    mine, theirs = pl.pallas_call(
        close_kernel,
        out_shape=(
            jax.ShapeDtypeStruct((tok, cols), jnp.float32),
            jax.ShapeDtypeStruct((tok, cols), jnp.bfloat16),
        ),
        in_specs=smem + in_vmem(3),
        out_specs=tuple(in_vmem(2)),
        compiler_params=limit,
    )(spots, part, tail, values[7])
    return (mine + swap_rows(theirs).astype(jnp.float32)).astype(jnp.bfloat16)


def body(tokens, w_query, w_keyval, w_out):
    tok_rows = tokens.shape[0]
    head = lax.axis_index("head").astype(jnp.int32)
    seq = lax.axis_index("seq").astype(jnp.int32)
    row, core = head >> 3, seq & 1
    spots = jnp.stack([head, core])
    half = w_query.shape[0] // 2
    quarter = half // 2
    kv_flat = w_keyval.T
    kv_part = swap_rows(lax.dynamic_slice_in_dim(kv_flat, (1 - row) * half, half, 1))
    q_same = swap_rows(
        lax.dynamic_slice_in_dim(w_query, (1 - row) * half + core * quarter, quarter, 0)
    )
    q_twin = other_core(q_same)
    kv_own = lax.dynamic_slice_in_dim(kv_flat, row * half, half, 1)
    shards, (piece, spots) = z_ring(tokens, (owned_piece(w_out, seq), spots))
    piece = lax.all_to_all(piece, "head", 0, 0, tiled=True, axis_index_groups=ROWS)
    kv_part, q_mine, q_theirs = project(
        spots,
        (*shards, kv_own, kv_part, w_query, q_same, q_twin),
        ((2 * kv_flat.shape[0], tok_rows),) + ((tok_rows, w_query.shape[1]),) * 2,
    )
    kv_sent = swap_rows(kv_part)
    piece, kv_sent = lax.optimization_barrier((piece, kv_sent))
    q_sent = swap_rows(q_theirs)
    keyval = sent_to_row(kv_part, kv_sent).reshape(8, 2, kv_flat.shape[0], tok_rows)
    near = along_seq(keyval, 1)
    far = along_seq(keyval[:, 0], 2)
    attended = attend(seq.reshape(1), q_mine, q_sent, far, near, keyval)
    values = z_ring(attended)
    held, twin, values[3] = owned_columns(piece, seq, values[3])
    return finish(spots, values, held, twin)


def solution(mesh):
    return jax.shard_map(
        body,
        mesh=mesh,
        in_specs=(P("seq", "head"), P(None, "head"), P(None, "head"), P("head", None)),
        out_specs=P("seq", "head"),
        check_vma=False,
    )
```

```python
import jax
import jax.numpy as jnp
from jax import lax
from jax.experimental import pallas as pl
from jax.experimental.pallas import tpu as pltpu
from jax.sharding import PartitionSpec as P


HEAD = 128
WIN1 = 512
WIN2 = 32
BLK = 128
GROUP = 32
MIX = 16
LOW = -1e30
LANES = (((1,), (1,)), ((), ()))


def pick(source, which, lanes):
    places = slice((which % 2) * 4, (which % 2) * 4 + 4)
    found = source[places, :, lanes] if len(source.shape) == 3 else source[places, which // 2, :, lanes]
    return found.reshape(HEAD, BLK)


def attend_kernel(
    seq_ref, mine_any, sent_any, far_ref, near_ref, own_ref, out_ref,
    k2f, v2f, ktile, vtile, kpair, vpair, s_scr, mx_scr, mcb_scr, mine_ref, sent_ref, sems,
):
    fetches = [
        pltpu.make_async_copy(source, target, sems.at[k])
        for k, (source, target) in enumerate(((mine_any, mine_ref), (sent_any, sent_ref)))
    ]
    for fetch in fetches:
        fetch.start()
    tok = mine_ref.shape[0]
    heads = mine_ref.shape[1] // HEAD
    blocks = tok // BLK
    seq = seq_ref[0]
    coef = (HEAD ** -0.5) * 1.4426950408889634
    start = seq == 0

    for t in range(6):
        source = (far_ref, near_ref, own_ref)[t // 2]
        lanes = slice((t % 2) * BLK, (t % 2 + 1) * BLK)
        ktile[t] = pick(source, 0, lanes)
        vtile[t] = pick(source, 1, lanes).astype(jnp.float32).T.astype(jnp.bfloat16)
    for scr, which in ((k2f, 2), (v2f, 3)):
        scr[:BLK] = pick(near_ref, which, slice(tok - BLK, tok)).astype(jnp.float32).T
        for t in range(blocks):
            scr[(t + 1) * BLK:(t + 2) * BLK] = pick(own_ref, which, slice(t * BLK, (t + 1) * BLK)).astype(jnp.float32).T

    @pl.when(start)
    def _():
        k2f[:BLK] = jnp.broadcast_to(k2f[BLK:BLK + 1], (BLK, HEAD))
        v2f[:BLK] = jnp.zeros((BLK, HEAD), jnp.float32)

    for fetch in fetches:
        fetch.wait()
    row = lax.broadcasted_iota(jnp.int32, (BLK, BLK), 0)
    col = lax.broadcasted_iota(jnp.int32, (BLK, BLK), 1)
    early = col > row
    absent = jnp.maximum(WIN1 - seq * tok, 0) // BLK

    def one(combo, _):
        h = combo // blocks
        b = combo % blocks
        base = pl.multiple_of(b * BLK, BLK)
        hcol = pl.multiple_of(h * HEAD, HEAD)
        at = (pl.ds(base, BLK), pl.ds(hcol, HEAD))
        qf = (mine_ref[at] + sent_ref[at]).astype(jnp.bfloat16).astype(jnp.float32)
        for slot, t in enumerate((0, 4, 1, 2, 3)):
            kpair[:, slot * BLK:(slot + 1) * BLK] = ktile[b + t]
            vpair[slot * BLK:(slot + 1) * BLK] = vtile[b + t]
        mx_scr[...] = jnp.full(mx_scr.shape, LOW, jnp.float32)

        def scores(step, _):
            lag0 = step * GROUP
            prods = []
            for g in range(GROUP):
                k2 = k2f[pl.ds(BLK + base - lag0 - g, BLK), :]
                prods.append((qf * k2).astype(jnp.bfloat16))
            prod = jnp.concatenate(prods, axis=0)
            for t in range(3):
                width = 2 * BLK if t < 2 else BLK
                s = jnp.dot(prod, kpair[:, 2 * BLK * t:2 * BLK * t + width], preferred_element_type=jnp.float32)
                s = s.reshape(GROUP, BLK, width)
                if t == 0:
                    parts = [(0, jnp.where(early[None], s[:, :, :BLK], s[:, :, BLK:]))]
                elif t == 1:
                    parts = [(1, s[:, :, :BLK]), (2, s[:, :, BLK:])]
                else:
                    parts = [(3, s)]
                for place, value in parts:
                    s_scr[pl.ds(lag0, GROUP), :, place * BLK:(place + 1) * BLK] = value
                    top = value[0]
                    for g in range(1, GROUP):
                        top = jnp.maximum(top, value[g])
                    mx_scr[place] = jnp.maximum(mx_scr[place], top)
            return 0

        lax.fori_loop(0, WIN2 // GROUP, scores, 0)
        tops = []
        gone = []
        for place in range(4):
            hide = (b + place) < absent
            mask = early if place == 0 else row >= 0
            gone.append(jnp.logical_and(mask, hide))
            tops.append(jnp.where(gone[place], LOW, mx_scr[place]))
        top = jnp.maximum(jnp.maximum(tops[0], tops[1]), jnp.maximum(tops[2], tops[3]))
        peak = jnp.max(top, axis=1, keepdims=True) * coef
        for place in range(4):
            mcb_scr[place] = jnp.where(gone[place], -LOW, jnp.broadcast_to(peak, (BLK, BLK)))

        def raised_at(lag):
            return [
                jnp.exp2(s_scr[lag, :, p * BLK:(p + 1) * BLK] * coef - mcb_scr[p])
                for p in range(4)
            ]

        def mix(step, carry):
            acc, tot = carry
            ws = []
            for g in range(MIX):
                raised = raised_at(step * MIX + g)
                tot = tot + ((raised[0] + raised[1]) + (raised[2] + raised[3]))
                split = [jnp.where(early, raised[0], 0.0), jnp.where(early, 0.0, raised[0])]
                ws.append(jnp.concatenate([part.astype(jnp.bfloat16) for part in split + raised[1:]], axis=1))
            m = jnp.dot(jnp.concatenate(ws, axis=0), vpair[...], preferred_element_type=jnp.float32)
            for g in range(MIX):
                acc = acc + m[g * BLK:(g + 1) * BLK] * v2f[pl.ds(BLK + base - step * MIX - g, BLK), :]
            return acc, tot

        zero = jnp.zeros((BLK, HEAD), jnp.float32)
        acc, tot = lax.fori_loop(0, WIN2 // MIX, mix, (zero, zero))
        last = raised_at(WIN2 - 1)
        spare = jnp.where(jnp.logical_and(start, b == 0), jnp.maximum(WIN2 - 1 - row, 0), 0)
        tot = tot - spare.astype(jnp.float32) * ((last[0] + last[1]) + (last[2] + last[3]))
        total = jnp.sum(tot, axis=1, keepdims=True)
        out_ref[at] = (acc / total).astype(jnp.bfloat16)
        return 0

    lax.fori_loop(0, heads * blocks, one, 0)


def in_vmem(count):
    return [pl.BlockSpec(memory_space=pltpu.VMEM)] * count


def attend(seq, mine, sent, far, near, own):
    tok = mine.shape[0]
    return pl.pallas_call(
        attend_kernel,
        out_shape=jax.ShapeDtypeStruct(mine.shape, jnp.bfloat16),
        in_specs=[pl.BlockSpec(memory_space=pltpu.SMEM)]
        + [pl.BlockSpec(memory_space=pltpu.HBM)] * 2
        + in_vmem(3),
        out_specs=in_vmem(1)[0],
        scratch_shapes=[
            pltpu.VMEM((BLK + tok, HEAD), jnp.float32),
            pltpu.VMEM((BLK + tok, HEAD), jnp.float32),
            pltpu.VMEM((6, HEAD, BLK), jnp.bfloat16),
            pltpu.VMEM((6, BLK, HEAD), jnp.bfloat16),
            pltpu.VMEM((HEAD, 5 * BLK), jnp.bfloat16),
            pltpu.VMEM((5 * BLK, HEAD), jnp.bfloat16),
            pltpu.VMEM((WIN2, BLK, 4 * BLK), jnp.float32),
            pltpu.VMEM((4, BLK, BLK), jnp.float32),
            pltpu.VMEM((4, BLK, BLK), jnp.float32),
            pltpu.VMEM(mine.shape, jnp.float32),
            pltpu.VMEM(mine.shape, jnp.float32),
            pltpu.SemaphoreType.DMA((2,)),
        ],
        compiler_params=pltpu.CompilerParams(vmem_limit_bytes=24 * 1024 * 1024),
    )(seq, mine, sent, far, near, own)


OFFSETS = (0, -1, 1, -2, 2, -3, 3, -4)


def at(place, count):
    return pl.ds(pl.multiple_of(place * count, count), count)


def fetch_all(moves, sems):
    fetches = [
        pltpu.make_async_copy(source, target, sems.at[k])
        for k, (source, target) in enumerate(moves)
    ]
    for fetch in fetches:
        fetch.start()
    return fetches


def into_rows(spot_ref, shards, rows_ref):
    depth = shards[0].shape[1]
    return [
        (source, rows_ref.at[:, at((spot_ref[0] + offset) & 7, depth)])
        for offset, source in zip(OFFSETS, shards)
    ]


def keyval_kernel(spot_ref, *refs):
    shards, kv_any, kv_out, rows_ref, kv_ref, sems = refs[:8], refs[8:10], *refs[10:]
    row = spot_ref[0] >> 3
    parts = kv_ref.shape[0] // 2
    moves = into_rows(spot_ref, shards, rows_ref)
    for source, side in zip(kv_any, (row, 1 - row)):
        moves.append((source, kv_ref.at[at(side, parts), :]))
    for fetch in fetch_all(moves, sems):
        fetch.wait()
    kv_out[...] = lax.dot_general(
        rows_ref[...], kv_ref[...], LANES, preferred_element_type=jnp.float32
    ).T


def query_kernel(spot_ref, *refs):
    shards, own_any, parts_any = refs[:8], refs[8], refs[9:11]
    mine_any, theirs_any, rows_ref, own_ref, part_ref, mine_out, theirs_out, sems = refs[11:]
    half = own_ref.shape[0]
    row, core = spot_ref[0] >> 3, spot_ref[1]
    moves = into_rows(spot_ref, shards, rows_ref)
    moves.append((own_any.at[at(row, half), :], own_ref))
    for source, side in zip(parts_any, (core, 1 - core)):
        moves.append((source, part_ref.at[at(side, half // 2), :]))
    fetches = fetch_all(moves, sems)
    for fetch in fetches[:9]:
        fetch.wait()
    mine_out[...] = jnp.dot(rows_ref[...], own_ref[...], preferred_element_type=jnp.float32)
    keep = pltpu.make_async_copy(mine_out, mine_any, sems.at[11])
    keep.start()
    for fetch in fetches[9:]:
        fetch.wait()
    theirs_out[...] = jnp.dot(rows_ref[...], part_ref[...], preferred_element_type=jnp.float32)
    send = pltpu.make_async_copy(theirs_out, theirs_any, sems.at[12])
    send.start()
    keep.wait()
    send.wait()


def project_keyval(spots, shards, kv_own, kv_part):
    tok, depth = shards[0].shape
    parts = kv_own.shape[0]
    return pl.pallas_call(
        keyval_kernel,
        out_shape=jax.ShapeDtypeStruct((2 * parts, tok), jnp.float32),
        in_specs=[pl.BlockSpec(memory_space=pltpu.SMEM)]
        + [pl.BlockSpec(memory_space=pltpu.HBM)] * 10,
        out_specs=in_vmem(1)[0],
        scratch_shapes=[
            pltpu.VMEM((tok, 8 * depth), kv_own.dtype),
            pltpu.VMEM((2 * parts, 8 * depth), kv_own.dtype),
            pltpu.SemaphoreType.DMA((10,)),
        ],
        compiler_params=pltpu.CompilerParams(vmem_limit_bytes=60 * 1024 * 1024),
    )(spots, *shards, kv_own, kv_part)


def project_query(spots, shards, own, same, twin):
    tok, depth = shards[0].shape
    far_off = pl.BlockSpec(memory_space=pltpu.HBM)
    half = (8 * depth, own.shape[1])
    out = jax.ShapeDtypeStruct((tok, own.shape[1]), jnp.float32)
    return pl.pallas_call(
        query_kernel,
        out_shape=(out, out),
        in_specs=[pl.BlockSpec(memory_space=pltpu.SMEM)] + [far_off] * 11,
        out_specs=(far_off, far_off),
        scratch_shapes=[
            pltpu.VMEM((tok, 8 * depth), own.dtype),
            pltpu.VMEM(half, own.dtype),
            pltpu.VMEM(half, own.dtype),
            pltpu.VMEM(out.shape, jnp.float32),
            pltpu.VMEM(out.shape, jnp.float32),
            pltpu.SemaphoreType.DMA((13,)),
        ],
        compiler_params=pltpu.CompilerParams(vmem_limit_bytes=60 * 1024 * 1024),
    )(spots, *shards, own, same, twin)


def swap_rows(value):
    return lax.ppermute(value, "head", [(i, (i + 8) % 16) for i in range(16)])


def along_z(value, step):
    return lax.ppermute(
        value, "head", [(i, (i // 8) * 8 + (i + step) % 8) for i in range(16)]
    )


def along_seq(value, step):
    return lax.ppermute(value, "seq", [(i, i + step) for i in range(16 - step)])


def round_x(value, step):
    return lax.ppermute(value, "seq", [(i, (i + 4 * step) % 16) for i in range(16)])


def other_core(value):
    return lax.ppermute(value, "seq", [(i, i ^ 1) for i in range(16)])


def z_ring(value, extra=None):
    found = [value]
    up = down = value
    for step in range(1, 5):
        up = along_z(up, 1)
        if step < 4:
            down = along_z(down, -1)
        if step < 4:
            if extra is not None and step == 2:
                up, down, *extra = lax.optimization_barrier((up, down, *extra))
            else:
                up, down = lax.optimization_barrier((up, down))
            found += [up, down]
        else:
            found.append(up)
    return found if extra is None else (found, extra)


ROWS = [list(range(8)), list(range(8, 16))]


def copies_kernel(one_ref, two_ref, out_ref):
    total = (one_ref[...] + two_ref[...]).astype(out_ref.dtype)
    for k in range(out_ref.shape[0]):
        out_ref[k] = total


def sent_to_row(one, two):
    copies = pl.pallas_call(
        copies_kernel,
        out_shape=jax.ShapeDtypeStruct((8, *one.shape), jnp.bfloat16),
        in_specs=in_vmem(2),
        out_specs=in_vmem(1)[0],
        compiler_params=pltpu.CompilerParams(vmem_limit_bytes=8 * 1024 * 1024),
    )(one, two)
    return lax.all_to_all(copies, "head", 0, 0, tiled=True, axis_index_groups=ROWS)


def owned_piece(w_out, seq):
    x, core = seq >> 2, seq & 1
    rows, width = w_out.shape
    part = rows // 8
    piece = lax.dynamic_slice_in_dim(w_out, (2 * x + core) * part, part, 0)
    return piece.reshape(part, 2, 8, width // 16).transpose(2, 1, 0, 3)


def owned_columns(piece, seq, tie):
    x = seq >> 2
    moved = [round_x(piece, step) for step in (1, 3, 2)]
    *moved, tie = lax.optimization_barrier((*moved, tie))
    held = jnp.zeros((4, *piece.shape), piece.dtype)
    held = lax.dynamic_update_slice_in_dim(held, piece[None], x, 0)
    for step, part in zip((1, 3, 2), moved):
        held = lax.dynamic_update_slice_in_dim(held, part[None], (x - step) & 3, 0)
    return held, other_core(held), tie


def gather_rows(spot_ref, held, twin, spot, out, slot):
    core = spot_ref[1]
    part = held.shape[3]
    cols = held.shape[4]
    for x in range(4):
        for source, side in ((held, core), (twin, 1 - core)):
            low = pl.multiple_of(x * 2 * part + side * part, part)
            for half in range(2):
                out[slot, pl.ds(low, part), half * cols:(half + 1) * cols] = source[x, spot, half]


def finish_kernel(spot_ref, *refs):
    values, held, twin = refs[:7], refs[7], refs[8]
    part_out, tail_out, w_scr = refs[9:]
    total = None
    for k, value in enumerate(values):
        gather_rows(spot_ref, held, twin, (spot_ref[0] + OFFSETS[k]) & 7, w_scr, k)
        new = jnp.dot(value[...], w_scr[k], preferred_element_type=jnp.float32)
        total = new if total is None else total + new
    part_out[...] = total
    gather_rows(spot_ref, held, twin, (spot_ref[0] + OFFSETS[7]) & 7, tail_out, 0)


def close_kernel(spot_ref, part_ref, tail_ref, last_ref, mine_out, theirs_out):
    total = part_ref[...] + jnp.dot(last_ref[...], tail_ref[0], preferred_element_type=jnp.float32)
    cols = mine_out.shape[1]
    for row in range(2):

        @pl.when((spot_ref[0] >> 3) == row)
        def _():
            mine_out[...] = total[:, row * cols:(row + 1) * cols]
            theirs_out[...] = total[:, (1 - row) * cols:(2 - row) * cols].astype(jnp.bfloat16)


def finish(spots, values, held, twin):
    tok, feats = values[0].shape
    cols = held.shape[-1]
    limit = pltpu.CompilerParams(vmem_limit_bytes=24 * 1024 * 1024)
    smem = [pl.BlockSpec(memory_space=pltpu.SMEM)]
    part, tail = pl.pallas_call(
        finish_kernel,
        out_shape=(
            jax.ShapeDtypeStruct((tok, 2 * cols), jnp.float32),
            jax.ShapeDtypeStruct((1, feats, 2 * cols), held.dtype),
        ),
        in_specs=smem + in_vmem(9),
        out_specs=tuple(in_vmem(2)),
        scratch_shapes=[pltpu.VMEM((7, feats, 2 * cols), held.dtype)],
        compiler_params=limit,
    )(spots, *values[:7], held, twin)
    mine, theirs = pl.pallas_call(
        close_kernel,
        out_shape=(
            jax.ShapeDtypeStruct((tok, cols), jnp.float32),
            jax.ShapeDtypeStruct((tok, cols), jnp.bfloat16),
        ),
        in_specs=smem + in_vmem(3),
        out_specs=tuple(in_vmem(2)),
        compiler_params=limit,
    )(spots, part, tail, values[7])
    return (mine + swap_rows(theirs).astype(jnp.float32)).astype(jnp.bfloat16)


def body(tokens, w_query, w_keyval, w_out):
    tok_rows = tokens.shape[0]
    head = lax.axis_index("head").astype(jnp.int32)
    seq = lax.axis_index("seq").astype(jnp.int32)
    row, core = head >> 3, seq & 1
    spots = jnp.stack([head, core])
    half = w_query.shape[0] // 2
    quarter = half // 2
    kv_flat = w_keyval.T
    kv_part = swap_rows(lax.dynamic_slice_in_dim(kv_flat, (1 - row) * half, half, 1))
    q_same = swap_rows(
        lax.dynamic_slice_in_dim(w_query, (1 - row) * half + core * quarter, quarter, 0)
    )
    q_twin = other_core(q_same)
    kv_own = lax.dynamic_slice_in_dim(kv_flat, row * half, half, 1)
    shards, (piece, spots) = z_ring(tokens, (owned_piece(w_out, seq), spots))
    piece = lax.all_to_all(piece, "head", 0, 0, tiled=True, axis_index_groups=ROWS)
    kv_part = project_keyval(spots, shards, kv_own, kv_part)
    q_mine, q_theirs = project_query(spots, shards, w_query, q_same, q_twin)
    kv_sent = swap_rows(kv_part)
    piece, kv_sent = lax.optimization_barrier((piece, kv_sent))
    q_sent = swap_rows(q_theirs)
    keyval = sent_to_row(kv_part, kv_sent).reshape(8, 2, kv_flat.shape[0], tok_rows)
    near = along_seq(keyval, 1)
    far = along_seq(keyval[:, 0], 2)
    attended = attend(seq.reshape(1), q_mine, q_sent, far, near, keyval)
    values = z_ring(attended)
    held, twin, values[3] = owned_columns(piece, seq, values[3])
    return finish(spots, values, held, twin)


def solution(mesh):
    return jax.shard_map(
        body,
        mesh=mesh,
        in_specs=(P("seq", "head"), P(None, "head"), P(None, "head"), P("head", None)),
        out_specs=P("seq", "head"),
        check_vma=False,
    )
```
